32 devices in a mesh: lat: 4 (over z), lon: 4 (over y, x), obs: 2 (over core).
Axes of the slice: x: 2, y: 2, z: 4, core: 2. Of those that a mesh axis runs over, the one named last changes fastest.
Arguments:
- innovation: float32 [4096, 128], P(('lat', 'lon', 'obs')), may hold values from -6 to 6
- obs_error: float32 [4096, 128], P(('lat', 'lon', 'obs')), may hold values from 0.5 to 2
- obs_offset: float32 [2, 4096, 128], P(None, ('lat', 'lon', 'obs')), may hold values from 0 to 1
- obs_cell: int32 [4096, 128], P(('lat', 'lon', 'obs')), may hold values from 0 to 65535
- obs_owner: int32 [32, 128], P(('lat', 'lon', 'obs')), may hold values from 0 to 15, as said below
- block_count: int32 [32], P(('lat', 'lon', 'obs')), may hold values from 64 to 128
- land_mask: int32 [256, 4096], P(('lat', 'obs'), 'lon'), may hold values from 0 to 1, as said below
- inertia: float32 [256, 4096], P(('lat', 'obs'), 'lon'), may hold values from 0.002 to 0.05
- sea_depth: float32 [256, 4096], P(('lat', 'obs'), 'lon'), may hold values from 0.5 to 5
Outputs:
- adjoint_field: float32 [256, 4096], P(('lat', 'obs'), 'lon')
- residual: float32 [256, 4096], P(('lat', 'obs'), 'lon')
The draws below stay inside these ranges and needn't reach their ends.
Inputs may be any that keep to these rules, and one draw needn't show every extreme that they name: `obs_owner`: among the live blocks of one device at most 16 name the same tile; in every draw some tile is named by exactly 16 live blocks of every device. `land_mask`: the first and the last grid row are land.
All inputs are finite; a program needn't handle non-finite values.
Results may differ from the reference program's by a relative error of at most 0.0003.
Values sent between devices are 32-bit elements; how exact they have to be, the bound alone decides.
A program may use at most 64 MiB of HBM per device.

```python
import math
import jax
import jax.numpy as jnp

TILE_R = 64
TILE_C = 1024
NBLK = 128
BLOCK = 128
ITERS = 5
CAPB = 16
NLAT = 256
NLON = 4096
N_LAT = 4
N_LON = 4
DEVICES = 32


def owner_plan(key):
    tile_count = N_LAT * N_LON
    slot_total = tile_count * CAPB
    base_key = jax.random.fold_in(key, 7711)
    block_counts = jax.random.randint(jax.random.fold_in(base_key, 1), (DEVICES,), NBLK // 2, NBLK + 1)
    hot_tile = jax.random.randint(jax.random.fold_in(base_key, 2), (), 0, tile_count)
    device_keys = jax.random.split(jax.random.fold_in(base_key, 3), DEVICES)

    def device_plan(dev_key, live_total):
        perm_key, mix_key = jax.random.split(dev_key)
        shuffled = jax.random.permutation(perm_key, slot_total)
        slot_ids = jnp.arange(slot_total)
        is_hot = slot_ids // CAPB == hot_tile
        sort_key = jnp.where(is_hot, slot_ids - slot_total, shuffled)
        chosen = jnp.argsort(sort_key)[:NBLK]
        owners = chosen // CAPB
        block_ids = jnp.arange(NBLK)
        mixing = jax.random.permutation(mix_key, NBLK)
        live_key = jnp.where(block_ids < live_total, mixing, NBLK + block_ids)
        return owners[jnp.argsort(live_key)]
    owners = jax.vmap(device_plan)(device_keys, block_counts)
    return (block_counts.astype(jnp.int32), owners.astype(jnp.int32))


def draw_obs_owner(key, part):
    return owner_plan(key)[1]


def draw_block_count(key, part):
    return owner_plan(key)[0]


def draw_land_mask(key, part):
    land_bits = jax.random.randint(jax.random.fold_in(key, 913), (NLAT, NLON), 0, 10)
    row_ids = jnp.arange(NLAT)[:, None]
    ocean = (land_bits < 7) & (row_ids > 0) & (row_ids < NLAT - 1)
    return ocean.astype(jnp.int32)


def touch_ends(result, rng, smallest, top_value):
    shape = result.shape
    index_at = [jax.random.randint(jax.random.fold_in(rng, axis), (), 0, shape[axis]) for axis in range(len(shape))]
    result = result.at[tuple(index_at)].set(smallest)
    longest = shape.index(max(shape))
    index_at[longest] = (index_at[longest] + 1) % shape[longest]
    return result.at[tuple(index_at)].set(top_value)


def block_levels(own_key, extent, cuts, smallest, high):
    level, own = 1.0, jax.random.fold_in(own_key, 6)
    for axis_at, blocks in cuts:
        steps = jnp.exp(jax.random.uniform(jax.random.fold_in(own, axis_at), (blocks,), jnp.float32, smallest / len(cuts), high / len(cuts)))
        level = level * jnp.repeat(steps, extent[axis_at] // blocks).reshape([-1 if axis == axis_at else 1 for axis in range(len(extent))])
    return level


def bell_draw(key, shape, deviation, limit, cuts=(), held_as=jnp.bfloat16):
    gain = block_levels(key, shape, cuts, -0.22, 0.18) if cuts else 1.0
    array = jax.random.normal(key, shape, jnp.float32) * deviation * gain
    return jnp.minimum(jnp.maximum(array, -limit), limit).astype(held_as)


def setup_inputs(seed: int = 0) -> dict:
    splits = jax.random.split(jax.random.key(seed), 10)
    return {
        "innovation": bell_draw(splits[0], (DEVICES * NBLK, BLOCK), 1.0, 6.0, ((0, 32),), jnp.float32),
        "obs_error": jnp.clip(jnp.exp(math.log(2.0) - 1.3862944 * jax.random.uniform(splits[1], (DEVICES * NBLK, BLOCK), jnp.float32) ** block_levels(splits[1], (DEVICES * NBLK, BLOCK), ((0, 32),), -0.2, 0.2)), 0.5, 2.0),
        "obs_offset": jnp.clip(1.0 * jax.random.uniform(splits[2], (2, DEVICES * NBLK, BLOCK), jnp.float32) ** block_levels(splits[2], (2, DEVICES * NBLK, BLOCK), ((1, 32),), -0.2, 0.2), 0.0, 1.0),
        "obs_cell": touch_ends(jax.random.randint(splits[3], (DEVICES * NBLK, BLOCK), 0, TILE_R * TILE_C), jax.random.fold_in(splits[3], 1), 0, (TILE_R * TILE_C) - 1).astype(jnp.int32),
        "obs_owner": draw_obs_owner(jax.random.fold_in(splits[9], 71), 0),
        "block_count": draw_block_count(jax.random.fold_in(splits[9], 71), 0),
        "land_mask": draw_land_mask(jax.random.fold_in(splits[9], 71), 0),
        "inertia": jnp.clip(jnp.exp(math.log(0.05) - 3.218876 * jax.random.uniform(splits[7], (NLAT, NLON), jnp.float32) ** block_levels(splits[7], (NLAT, NLON), ((0, 8), (1, 4)), -0.2, 0.2)), 0.002, 0.05),
        "sea_depth": jnp.clip(jnp.exp(math.log(5.0) - 2.3025851 * jax.random.uniform(splits[8], (NLAT, NLON), jnp.float32) ** block_levels(splits[8], (NLAT, NLON), ((0, 8), (1, 4)), -0.2, 0.2)), 0.5, 5.0),
    }


def reference(innovation, obs_error, obs_offset, obs_cell, obs_owner, block_count, land_mask, inertia, sea_depth):
    is_live = (jnp.arange(NBLK)[None, :] < block_count[:, None]).reshape(-1)
    owner_tile = obs_owner.reshape(-1)
    scaled = jnp.where(is_live[:, None], innovation / (obs_error * obs_error), jnp.float32(0.0))
    north_frac = obs_offset[0]
    east_frac = obs_offset[1]
    cell_row = (owner_tile // N_LON)[:, None] * TILE_R + obs_cell // TILE_C
    cell_col = (owner_tile % N_LON)[:, None] * TILE_C + obs_cell % TILE_C
    next_col = (cell_col + 1) % NLON
    next_row = cell_row + 1
    cell_total = NLAT * NLON
    inside = next_row < NLAT
    segment_ids = jnp.concatenate([(cell_row * NLON + cell_col).reshape(-1), (cell_row * NLON + next_col).reshape(-1), jnp.where(inside, next_row * NLON + cell_col, cell_total).reshape(-1), jnp.where(inside, next_row * NLON + next_col, cell_total).reshape(-1)]).astype(jnp.int32)
    contribs = jnp.concatenate([(scaled * ((1.0 - north_frac) * (1.0 - east_frac))).reshape(-1), (scaled * ((1.0 - north_frac) * east_frac)).reshape(-1), (scaled * (north_frac * (1.0 - east_frac))).reshape(-1), (scaled * (north_frac * east_frac)).reshape(-1)])
    partial_value = jax.ops.segment_sum(contribs, segment_ids, num_segments=cell_total + 1)[:cell_total]
    ocean = land_mask.astype(jnp.float32)
    forcing = partial_value.reshape(NLAT, NLON) * ocean
    conduct = ocean * sea_depth
    cond_north = jnp.sqrt(conduct * jnp.roll(conduct, 1, 0))
    cond_south = jnp.sqrt(conduct * jnp.roll(conduct, -1, 0))
    cond_west = jnp.sqrt(conduct * jnp.roll(conduct, 1, 1))
    cond_east = jnp.sqrt(conduct * jnp.roll(conduct, -1, 1))
    diagonal = inertia + cond_north + cond_south + cond_west + cond_east

    def operate(field):
        return diagonal * field - cond_north * jnp.roll(field, 1, 0) - cond_south * jnp.roll(field, -1, 0) - cond_west * jnp.roll(field, 1, 1) - cond_east * jnp.roll(field, -1, 1)
    adjoint_field = jnp.zeros_like(forcing)
    residual = forcing
    direction = forcing
    norm_now = jnp.sum(residual * residual)
    for iteration in range(ITERS):
        applied = operate(direction)
        step_size = norm_now / jnp.sum(direction * applied)
        adjoint_field = adjoint_field + step_size * direction
        residual = residual - step_size * applied
        norm_next = jnp.sum(residual * residual)
        direction = residual + norm_next / norm_now * direction
        norm_now = norm_next
    return (adjoint_field, residual)
```

```python
import functools

import jax
import jax.numpy as jnp
from jax import lax
from jax.experimental import pallas as pl
from jax.experimental.pallas import tpu as pltpu
from jax.sharding import PartitionSpec as P

ITERS = 5
ROW_PAD = 8
COL_PAD = 128
FINE_ROW = 16
FINE_COL = 8
MESH = pl.DeviceIdType.MESH
AXES = ("lat", "lon", "obs")
F32 = jnp.float32
BF16 = jnp.bfloat16


def iota(shape, axis):
    return lax.broadcasted_iota(jnp.int32, shape, axis)


def moved(value, axis, back):
    size = value.shape[axis]
    return pltpu.roll(value, size - 1 if back else 1, axis)


def fine_size():
    return -(-(FINE_ROW + 1) * (FINE_COL + 1) // 16) * 16


def spread_block(capacity, width, cols, coarse, block):
    fine = fine_size()
    amount = block[:, :width]
    north = block[:, width : 2 * width]
    east = block[:, 2 * width : 3 * width]
    cell = block[:, 3 * width :]
    row = jnp.floor(cell * (1.0 / cols))
    col = cell - row * cols
    row_group = jnp.floor(row * (1.0 / FINE_ROW))
    col_group = jnp.floor(col * (1.0 / FINE_COL))
    step = FINE_ROW + 1
    first = (col - col_group * FINE_COL) * step + (row - row_group * FINE_ROW)
    group = row_group * (cols // FINE_COL) + col_group - coarse // 2
    upper = amount * (1.0 - north)
    lower = amount * north
    corners = []
    for shift, part in (
        (0, upper * (1.0 - east)),
        (1, lower * (1.0 - east)),
        (step, upper * east),
        (step + 1, lower * east),
    ):
        high = part.astype(BF16).astype(F32)
        corners.append((first + shift, high, part - high))

    def wide(values, slot, count):
        tile = jnp.broadcast_to(values[slot : slot + 1], (16, width)).astype(BF16)
        return jnp.concatenate([tile] * (count // 16), axis=0)

    fine_axis = iota((fine, width), 0).astype(F32).astype(BF16)
    coarse_axis = (iota((coarse, width), 0) - coarse // 2).astype(F32).astype(BF16)
    zero = jnp.zeros((), BF16)
    one = jnp.ones((), BF16)
    left, right = [], []
    for slot in range(capacity):
        high = low = zero
        for place, top, rest in corners:
            hit = fine_axis == wide(place, slot, fine)
            high = jnp.where(hit, wide(top, slot, fine), high)
            low = jnp.where(hit, wide(rest, slot, fine), low)
        left.append(jnp.concatenate([high, low], axis=0))
        right.append(jnp.where(coarse_axis == wide(group, slot, coarse), one, zero))
    return lax.dot_general(
        jnp.concatenate(left, axis=1),
        jnp.concatenate(right, axis=1),
        (((1,), (1,)), ((), ())),
        preferred_element_type=F32,
    )


def kernel(
    capacity,
    innov_hbm, error_hbm, offset_hbm, cell_hbm, owner_hbm, count_ref, land_hbm, inertia_hbm, depth_hbm,
    x_ref, r_ref,
    innov_ref, error_ref, offset_ref, cell_ref, owner_ref, land_ref, depth_ref, ground_ref,
    sent_ref, inbox_ref, acc_ref, perm_ref,
    tile_ref, pack_ref, strip_ref, pair_ref, edge_ref, side_ref,
    up_ref, down_ref, mid_ref, cwest_ref, ceast_ref,
    ocean_ref, diag_ref, cn_ref, cs_ref, cw_ref, ce_ref, q_ref,
    part_ref, slot_ref, gram_ref,
    in_sem, send_sem, recv_sem, halo_send, halo_recv, swap_send, swap_recv, sum_send, sum_recv,
):
    n_lat, n_lon, n_obs = (lax.axis_size(name) for name in AXES)
    lat, lon, core = (lax.axis_index(name) for name in AXES)
    tiles = n_lat * n_lon
    total = tiles * n_obs
    me = (lat * n_lon + lon) * n_obs + core
    rows, cols = x_ref.shape
    tall = rows + 2 * ROW_PAD
    keep = rows + ROW_PAD
    tile_rows = rows * n_obs
    blocks, width = innov_ref.shape
    cap_pad = sent_ref.shape[1]
    fine = fine_size()
    coarse = acc_ref.shape[1]
    group_cols = cols // FINE_COL

    def place(flat):
        return (flat // (n_lon * n_obs), (flat // n_obs) % n_lon, flat % n_obs)

    loads = [
        pltpu.make_async_copy(source, target, in_sem.at[number])
        for number, (source, target) in enumerate(
            (
                (owner_hbm, owner_ref),
                (innov_hbm, innov_ref),
                (error_hbm, error_ref),
                (offset_hbm, offset_ref),
                (cell_hbm, cell_ref),
                (land_hbm, land_ref),
                (depth_hbm, depth_ref),
                (inertia_hbm, ground_ref.at[1]),
            )
        )
    ]
    for load in loads:
        load.start()

    barrier = pltpu.get_barrier_semaphore()

    def greet(k, carry):
        pl.semaphore_signal(
            barrier, inc=1, device_id=place(lax.rem(me + k, total)), device_id_type=MESH
        )
        return carry

    lax.fori_loop(1, total, greet, 0)

    loads[0].wait()
    count = count_ref[0]
    owner_row = jnp.broadcast_to(owner_ref[...].astype(F32), (blocks, blocks))
    owner_col = owner_row.T
    earlier = (iota((blocks, blocks), 0) < iota((blocks, blocks), 1)) & (
        iota((blocks, blocks), 0) < count
    )
    same = jnp.where((owner_row == owner_col) & earlier, 1.0, 0.0)
    rank = jnp.sum(same, axis=0, keepdims=True)
    slot_of = owner_row[:1] * cap_pad + rank
    slot_of = jnp.where(iota((1, blocks), 1) < count, slot_of, -1.0)
    slots = tiles * cap_pad
    chosen = iota((slots, blocks), 0).astype(F32) == slot_of
    chosen = jnp.where(chosen, 1.0, 0.0).astype(BF16)
    for load in loads[1:5]:
        load.wait()
    error = error_ref[...]
    data = jnp.concatenate(
        [
            innov_ref[...] / (error * error),
            offset_ref[0],
            offset_ref[1],
            cell_ref[...].astype(F32),
        ],
        axis=1,
    )
    high = data.astype(BF16)
    rest = data - high.astype(F32)
    middle = rest.astype(BF16)
    low = (rest - middle.astype(F32)).astype(BF16)
    sent_ref[...] = jnp.dot(
        jnp.concatenate([chosen] * 3, axis=1),
        jnp.concatenate([high, middle, low], axis=0),
        preferred_element_type=F32,
    ).reshape(sent_ref.shape)
    for load in loads[5:]:
        load.wait()
    ground_ref[0] = land_ref[...].astype(F32) * depth_ref[...]
    pl.semaphore_wait(barrier, total - 1)

    def turn_of(k):
        ring_step, shift = k // n_lon, k % n_lon
        odd = ring_step % 2
        hop = odd * ((ring_step + 1) // 2) + (1 - odd) * (n_lat - ring_step // 2)
        return hop % n_lat, shift

    def block_copy(k):
        hop, shift = turn_of(k)
        to_lat, to_lon = (lat + hop) % n_lat, (lon + shift) % n_lon
        return pltpu.make_async_remote_copy(
            src_ref=sent_ref.at[to_lat * n_lon + to_lon],
            dst_ref=inbox_ref.at[k],
            send_sem=send_sem.at[k],
            recv_sem=recv_sem.at[k],
            device_id=(to_lat, to_lon, core),
            device_id_type=MESH,
        )

    def send(k, carry):
        block_copy(tiles - k).start()
        return carry

    lax.fori_loop(1, tiles, send, 0)

    def halo_copy(index, source, target, device):
        return pltpu.make_async_remote_copy(
            src_ref=source,
            dst_ref=target,
            send_sem=halo_send.at[index],
            recv_sem=halo_recv.at[index],
            device_id=device,
            device_id_type=MESH,
        )

    ring = n_lat * n_obs
    line = lat * n_obs + core
    above = lax.rem(line + ring - 1, ring)
    below = lax.rem(line + 1, ring)
    west = lax.rem(lon + n_lon - 1, n_lon)
    east = lax.rem(lon + 1, n_lon)
    to_below = halo_copy(
        0, ground_ref.at[:, pl.ds(rows - ROW_PAD, ROW_PAD)], up_ref, (below // n_obs, lon, below % n_obs)
    )
    to_above = halo_copy(
        1, ground_ref.at[:, pl.ds(0, ROW_PAD)], down_ref, (above // n_obs, lon, above % n_obs)
    )
    to_east = halo_copy(2, mid_ref.at[:, :, pl.ds(cols - COL_PAD, COL_PAD)], cwest_ref, (lat, east, core))
    to_west = halo_copy(3, mid_ref.at[:, :, pl.ds(0, COL_PAD)], ceast_ref, (lat, west, core))
    to_below.start()
    to_above.start()

    def post_sum(turn, parts):
        stack = jnp.concatenate(
            parts + [jnp.zeros((COL_PAD - 8 * len(parts), COL_PAD), F32)], axis=0
        )
        values = jnp.sum(stack.T, axis=0, keepdims=True)
        slot_ref[turn, pl.ds(me, 1)] = values[None]
        part_ref[turn] = values

        def post(k, carry):
            pltpu.make_async_remote_copy(
                src_ref=part_ref.at[turn],
                dst_ref=slot_ref.at[turn, me],
                send_sem=sum_send.at[turn],
                recv_sem=sum_recv.at[turn],
                device_id=place(lax.rem(me + k, total)),
                device_id_type=MESH,
            ).start()
            return carry

        lax.fori_loop(1, total, post, 0)

    def take_sum(turn, number):
        block = slot_ref.at[turn, pl.ds(0, total - 1)]
        pltpu.make_async_copy(block, block, sum_recv.at[turn]).wait()
        pltpu.make_async_copy(block, block, sum_send.at[turn]).wait()
        values = jnp.sum(slot_ref[turn], axis=0)
        gram_ref[...] = jnp.broadcast_to(values, (COL_PAD, COL_PAD)).T
        return [
            jnp.sum(gram_ref[8 * k : 8 * k + 8], axis=0, keepdims=True) for k in range(number)
        ]

    def inner(value):
        return value[ROW_PAD:keep, :cols]

    def fold(value):
        out = value[:8]
        for start in range(8, rows, 8):
            out = out + value[start : start + 8]
        lanes = out[:, :COL_PAD]
        for start in range(COL_PAD, cols, COL_PAD):
            lanes = lanes + out[:, start : start + COL_PAD]
        return lanes

    def spread(k):
        return spread_block(capacity, width, cols, coarse, k)

    acc_ref[...] = spread(sent_ref[lat * n_lon + lon])

    def fill(part, carry):
        shape = (group_cols, cols)
        target = iota(shape, 0) * FINE_COL + part
        start = pl.multiple_of(part * group_cols, group_cols)
        perm_ref[pl.ds(start, group_cols)] = jnp.where(target == iota(shape, 1), 1.0, 0.0).astype(BF16)
        return carry

    lax.fori_loop(0, FINE_COL, fill, 0)

    def turn(k, carry):
        block_copy(k).wait_recv()
        acc_ref[...] = acc_ref[...] + spread(inbox_ref[k])

        @pl.when(k == tiles // 4 - 1)
        def _():
            to_below.wait()
            to_above.wait()
            mid_ref[:, :ROW_PAD] = up_ref[...]
            mid_ref[:, ROW_PAD:keep] = ground_ref[...]
            mid_ref[:, keep:] = down_ref[...]
            to_east.start()
            to_west.start()

        @pl.when(k == tiles // 2 - 1)
        def _():
            to_east.wait()
            to_west.wait()
            near = iota((tall, COL_PAD), 1) < COL_PAD // 2

            def widened(index):
                pad = jnp.where(near, ceast_ref[index], cwest_ref[index])
                return jnp.concatenate([mid_ref[index], pad], axis=1)

            conduct = widened(0)
            cn = jnp.sqrt(conduct * moved(conduct, 0, False))
            cs = moved(cn, 0, True)
            cw = jnp.sqrt(conduct * moved(conduct, 1, False))
            ce = moved(cw, 1, True)
            ocean = jnp.where(conduct > 0.0, 1.0, 0.0)
            diag = widened(1) + cn + cs + cw + ce
            cn_ref[...] = cn
            cs_ref[...] = cs
            cw_ref[...] = cw
            ce_ref[...] = ce
            ocean_ref[...] = ocean
            diag_ref[...] = diag
            kept = inner(diag) * inner(ocean)
            faces = cn * cn + cs * cs + cw * cw + ce * ce
            post_sum(0, [fold(inner(ocean)), fold(kept), fold(kept * kept), fold(inner(faces))])

        return carry

    lax.fori_loop(1, tiles, turn, 0)

    acc_ref[:fine] = acc_ref[:fine] + acc_ref[fine:]
    step = FINE_ROW + 1
    top_row = iota((8, group_cols), 0) == 0
    blank = jnp.zeros((FINE_ROW - 8, group_cols), F32)
    planes = []
    for part in range(FINE_COL + 1):
        pieces, spill = [], None
        for index in range(tile_rows // FINE_ROW):
            lanes = slice(index * group_cols, (index + 1) * group_cols)
            piece = acc_ref[part * step : part * step + FINE_ROW, lanes]
            if spill is not None:
                piece = piece + jnp.concatenate([spill, blank], axis=0)
            pieces.append(piece)
            last = acc_ref[part * step + FINE_ROW : part * step + step, lanes]
            spill = jnp.where(top_row, last, 0.0)
        planes.append(jnp.concatenate(pieces + [spill], axis=0))
    over = pltpu.roll(planes[FINE_COL], 1, 1)
    lane = iota(over.shape, 1)
    planes[0] = planes[0] + jnp.where(lane > 0, over, 0.0)
    beyond = jnp.where(lane == 0, over, 0.0)
    mixed = jnp.concatenate(planes[:FINE_COL], axis=1)
    high = mixed.astype(BF16).astype(F32)
    mixed = jnp.concatenate([high, mixed - high], axis=0).astype(BF16)
    natural = jnp.dot(mixed, perm_ref[...], preferred_element_type=F32)
    tile_tall = tile_rows + ROW_PAD
    natural = natural[:tile_tall] + natural[tile_tall:]
    tile_ref[:, :cols] = natural
    tile_ref[:, cols:] = beyond
    top = iota((ROW_PAD, cols + COL_PAD), 0) == 0
    pack_ref[...] = jnp.where(
        top, tile_ref[tile_rows:], tile_ref[tile_rows - ROW_PAD : tile_rows]
    )
    sides = jnp.where(lane < COL_PAD // 2, natural[:, :COL_PAD], natural[:, cols - COL_PAD :])
    sides = jnp.where(lane == COL_PAD - 8, pltpu.roll(beyond, COL_PAD - 8, 1), sides)
    sides = jnp.concatenate([sides, jnp.zeros((COL_PAD - tile_tall, COL_PAD), F32)], axis=0)
    strip_ref[...] = sides.T

    split = rows - ROW_PAD
    mine = pl.multiple_of(core * split, 8)
    theirs = pl.multiple_of((1 - core) * split, 8)
    north = lat > 0
    south = lat < n_lat - 1
    from_west = strip_ref.at[pl.ds(0, 8)]
    from_east = strip_ref.at[pl.ds(COL_PAD - 8, 8)]

    def swap_copy(out, into, source, target, device):
        return pltpu.make_async_remote_copy(
            src_ref=source,
            dst_ref=target,
            send_sem=swap_send.at[out],
            recv_sem=swap_recv.at[into],
            device_id=device,
            device_id_type=MESH,
        )

    up_lat, down_lat = jnp.maximum(lat - 1, 0), jnp.minimum(lat + 1, n_lat - 1)

    def northern():
        return [
            swap_copy(1, 1 + core, tile_ref.at[pl.ds(0, 8)], edge_ref.at[core], (up_lat, lon, 1)),
            swap_copy(2, 3 + core, from_west, side_ref.at[2 + core], (up_lat, west, 1)),
            swap_copy(3, 5 + core, from_east, side_ref.at[6 + core], (up_lat, east, 1)),
        ]

    def southern():
        return [
            swap_copy(4, 1 + core, pack_ref, edge_ref.at[core], (down_lat, lon, 0)),
            swap_copy(5, 3 + core, from_west, side_ref.at[2 + core], (down_lat, west, 0)),
            swap_copy(6, 5 + core, from_east, side_ref.at[6 + core], (down_lat, east, 0)),
        ]

    level = [
        swap_copy(7 + peer, 7 + core, from_west, side_ref.at[core], (lat, west, peer))
        for peer in range(2)
    ] + [
        swap_copy(9 + peer, 9 + core, from_east, side_ref.at[4 + core], (lat, east, peer))
        for peer in range(2)
    ]
    swap = swap_copy(0, 0, tile_ref.at[pl.ds(theirs, tall)], pair_ref, (lat, lon, 1 - core))

    @pl.when(north)
    def _():
        for item in northern():
            item.start()

    @pl.when(south)
    def _():
        for item in southern():
            item.start()

    for item in level:
        item.start()
    swap.start()

    ocean_count, diag_sum, diag_square, face_square = take_sum(0, 4)
    ocean_count = jnp.maximum(ocean_count, 1.0)
    mean = diag_sum / ocean_count
    spread_out = jnp.maximum((diag_square + face_square) / ocean_count - mean * mean, 0.0)
    mean = 1.2 * mean

    def across(value, size):
        return jnp.concatenate([value] * (size // COL_PAD), axis=1)

    diag_ref[...] = diag_ref[...] - across(mean, cols + COL_PAD)

    linked = jnp.where(core == 0, lat, n_lat - 1 - lat) > 0

    def arrived(number, target):
        return swap_copy(0, number, target, target, (lat, lon, 1 - core))

    @pl.when(linked)
    def _():
        for sender in range(2):
            arrived(1 + sender, edge_ref.at[sender]).wait_recv()
            arrived(3 + sender, side_ref.at[2 + sender]).wait_recv()
            arrived(5 + sender, side_ref.at[6 + sender]).wait_recv()

    @pl.when(jnp.logical_not(linked))
    def _():
        edge_ref[...] = jnp.zeros_like(edge_ref)
        side_ref[2:4] = jnp.zeros((2, 8, COL_PAD), F32)
        side_ref[6:8] = jnp.zeros((2, 8, COL_PAD), F32)

    for sender in range(2):
        arrived(7 + sender, side_ref.at[sender]).wait_recv()
        arrived(9 + sender, side_ref.at[4 + sender]).wait_recv()

    def aligned(straight, corner):
        first = core == 0
        straight = jnp.where(
            first, pltpu.roll(straight, ROW_PAD, 1), pltpu.roll(straight, COL_PAD - split, 1)
        )
        corner = jnp.where(
            first,
            pltpu.roll(corner, COL_PAD - (tile_rows - ROW_PAD), 1),
            pltpu.roll(corner, keep, 1),
        )
        return straight + corner

    right_side = aligned(side_ref[0] + side_ref[1], side_ref[2] + side_ref[3])
    left_side = aligned(side_ref[4] + side_ref[5], side_ref[6] + side_ref[7])
    hole = jnp.zeros((COL_PAD - 16, COL_PAD), F32)
    beside = jnp.concatenate([right_side, hole, left_side], axis=0).T[:tall]
    entering = jnp.where(iota(beside.shape, 1) == 0, pltpu.roll(beside, 8, 1), 0.0)
    edge = edge_ref[0] + edge_ref[1]
    swap.wait_recv()

    @pl.when(core == 0)
    def _():
        q_ref[0, :ROW_PAD] = jnp.where(top, 0.0, edge)
        q_ref[0, ROW_PAD : 2 * ROW_PAD] = (
            tile_ref[:ROW_PAD] + pair_ref[:ROW_PAD] + jnp.where(top, edge, 0.0)
        )
        q_ref[0, 2 * ROW_PAD :] = tile_ref[ROW_PAD:keep] + pair_ref[ROW_PAD:keep]

    @pl.when(core == 1)
    def _():
        q_ref[0, :keep] = tile_ref[pl.ds(split, keep)] + pair_ref[:keep]
        q_ref[0, keep:] = tile_ref[pl.ds(split + keep, ROW_PAD)] + pair_ref[keep:] + edge

    q_ref[0, :, :COL_PAD] = q_ref[0, :, :COL_PAD] + entering
    q_ref[0, :, cols:] = q_ref[0, :, cols:] + beside
    q_ref[0] = q_ref[0] * ocean_ref[...]

    spread_wide = across(spread_out, cols + COL_PAD)
    for k in range(ITERS):
        field = q_ref[k]
        value = (
            diag_ref[...] * field
            - cn_ref[...] * moved(field, 0, False)
            - cs_ref[...] * moved(field, 0, True)
            - cw_ref[...] * moved(field, 1, False)
            - ce_ref[...] * moved(field, 1, True)
        )
        if k:
            value = value - spread_wide * q_ref[k - 1]
        q_ref[k + 1] = value

    fields = [q_ref[k, ROW_PAD:keep, :cols] for k in range(ITERS + 1)]
    pairs = [(k, k + d) for k in range(ITERS) for d in range(2)]
    post_sum(1, [fold(fields[i] * fields[j]) for i, j in pairs])
    sums = take_sum(1, len(pairs))
    gram = {}
    for (i, j), value in zip(pairs, sums):
        gram[i, j] = gram[j, i] = value
    for gap in range(1, ITERS):
        for i in range(ITERS - gap):
            j = i + gap
            value = gram[i + 1, j]
            if i:
                value = value + spread_out * (gram[i - 1, j] - gram[i, j - 1])
            else:
                value = value - spread_out * gram[i, j - 1]
            gram[i, j + 1] = gram[j + 1, i] = value

    def plus(one, two):
        if one is None or two is None:
            return two if one is None else one
        return one + two

    def times(weight, part):
        return None if part is None else weight * part

    def quad(first, second):
        out = None
        for i, one in enumerate(first):
            line = None
            for j, two in enumerate(second):
                if one is not None and two is not None:
                    line = plus(line, two * gram[i, j])
            out = plus(out, times(one, line) if one is not None else None)
        return out

    def apply(weights):
        out = [None] * (ITERS + 1)
        for k, weight in enumerate(weights[:ITERS]):
            if weight is not None:
                out[k + 1] = plus(out[k + 1], weight)
                out[k] = plus(out[k], mean * weight)
                if k:
                    out[k - 1] = plus(out[k - 1], spread_out * weight)
        return out

    unit = jnp.ones((1, COL_PAD), F32)
    direct = [unit] + [None] * ITERS
    resid = [unit] + [None] * ITERS
    gained = [None] * (ITERS + 1)
    norm = gram[0, 0]
    for done in range(1, ITERS + 1):
        applied = apply(direct)
        step_size = norm / quad(direct, applied)
        gained = [plus(one, times(step_size, two)) for one, two in zip(gained, direct)]
        resid = [plus(one, times(-step_size, two)) for one, two in zip(resid, applied)]
        if done < ITERS:
            norm_next = quad(resid, resid)
            ratio = norm_next / norm
            direct = [plus(one, times(ratio, two)) for one, two in zip(resid, direct)]
            norm = norm_next

    def mix(weights):
        out = None
        for k, weight in enumerate(weights):
            if weight is not None:
                out = plus(out, across(weight, cols) * q_ref[k, ROW_PAD:keep, :cols])
        return out

    x_ref[...] = mix(gained)
    r_ref[...] = mix(resid)

    def finish(k, carry):
        block_copy(k).wait_send()
        return carry

    lax.fori_loop(1, tiles, finish, 0)
    swap.wait_send()
    for item in level:
        item.wait_send()

    @pl.when(north)
    def _():
        for item in northern():
            item.wait_send()

    @pl.when(south)
    def _():
        for item in southern():
            item.wait_send()


def body(
    innovation, obs_error, obs_offset, obs_cell, obs_owner, block_count,
    land_mask, inertia, sea_depth,
):
    block_total = obs_owner.shape[1]
    width = innovation.shape[1]
    n_lat, n_lon, n_obs = (lax.axis_size(name) for name in AXES)
    tiles = n_lat * n_lon
    capacity = max(3, 2 * ((block_total + tiles - 1) // tiles))
    cap_pad = -(-capacity // 8) * 8
    rows, cols = land_mask.shape
    total = tiles * n_obs
    coarse = (rows * n_obs // FINE_ROW) * (cols // FINE_COL)
    tall, broad = rows + 2 * ROW_PAD, cols + COL_PAD
    tile_tall = rows * n_obs + ROW_PAD
    vmem = lambda *shape: pltpu.VMEM(shape, F32)
    whole = pl.BlockSpec(memory_space=pltpu.VMEM)
    far = pl.BlockSpec(memory_space=pltpu.HBM)
    near = pl.BlockSpec(memory_space=pltpu.SMEM)
    dma = pltpu.SemaphoreType.DMA
    return pl.pallas_call(
        functools.partial(kernel, capacity),
        out_shape=[jax.ShapeDtypeStruct((rows, cols), F32)] * 2,
        in_specs=[far] * 5 + [near] + [far] * 3,
        out_specs=[whole] * 2,
        scratch_shapes=[
            vmem(*innovation.shape),
            vmem(*obs_error.shape),
            vmem(*obs_offset.shape),
            pltpu.VMEM(obs_cell.shape, jnp.int32),
            pltpu.VMEM(obs_owner.shape, jnp.int32),
            pltpu.VMEM((rows, cols), jnp.int32),
            vmem(rows, cols),
            vmem(2, rows, cols),
            vmem(tiles, cap_pad, 4 * width),
            vmem(tiles, cap_pad, 4 * width),
            vmem(2 * fine_size(), coarse),
            pltpu.VMEM((cols, cols), BF16),
            vmem(tile_tall, broad),
            vmem(ROW_PAD, broad),
            vmem(COL_PAD, COL_PAD),
            vmem(tall, broad),
            vmem(2, ROW_PAD, broad),
            vmem(8, 8, COL_PAD),
            vmem(2, ROW_PAD, cols),
            vmem(2, ROW_PAD, cols),
            vmem(2, tall, cols),
            vmem(2, tall, COL_PAD),
            vmem(2, tall, COL_PAD),
        ]
        + [vmem(tall, broad)] * 6
        + [
            vmem(ITERS + 1, tall, broad),
            vmem(2, 1, COL_PAD),
            vmem(2, total, 1, COL_PAD),
            vmem(COL_PAD, COL_PAD),
            dma((8,)),
            dma((tiles,)),
            dma((tiles,)),
            dma((4,)),
            dma((4,)),
            dma((11,)),
            dma((11,)),
            dma((2,)),
            dma((2,)),
        ],
        compiler_params=pltpu.CompilerParams(collective_id=0, has_side_effects=True),
        name="adjoint",
    )(
        innovation, obs_error, obs_offset, obs_cell, obs_owner, block_count,
        land_mask, inertia, sea_depth,
    )


def solution(mesh):
    spread = P(AXES, None)
    grid = P(("lat", "obs"), "lon")
    in_specs = (spread, spread, P(None, AXES, None), spread, spread, P(AXES), grid, grid, grid)
    return jax.shard_map(
        body, mesh=mesh, in_specs=in_specs, out_specs=(grid, grid), check_vma=False
    )
```

```python
import functools

import jax
import jax.numpy as jnp
from jax import lax
from jax.experimental import pallas as pl
from jax.experimental.pallas import tpu as pltpu
from jax.sharding import PartitionSpec as P

ITERS = 5
ROW_PAD = 8
COL_PAD = 128
FINE_ROW = 16
FINE_COL = 8
MESH = pl.DeviceIdType.MESH
AXES = ("lat", "lon", "obs")
F32 = jnp.float32
BF16 = jnp.bfloat16


def iota(shape, axis):
    return lax.broadcasted_iota(jnp.int32, shape, axis)


def moved(value, axis, back):
    size = value.shape[axis]
    return pltpu.roll(value, size - 1 if back else 1, axis)


def fine_size():
    return -(-(FINE_ROW + 1) * (FINE_COL + 1) // 16) * 16


def spread_block(capacity, width, cols, coarse, block):
    fine = fine_size()
    amount = block[:, :width]
    north = block[:, width : 2 * width]
    east = block[:, 2 * width : 3 * width]
    cell = block[:, 3 * width :]
    row = jnp.floor(cell * (1.0 / cols))
    col = cell - row * cols
    row_group = jnp.floor(row * (1.0 / FINE_ROW))
    col_group = jnp.floor(col * (1.0 / FINE_COL))
    step = FINE_ROW + 1
    first = (col - col_group * FINE_COL) * step + (row - row_group * FINE_ROW)
    group = row_group * (cols // FINE_COL) + col_group - coarse // 2
    upper = amount * (1.0 - north)
    lower = amount * north
    corners = []
    for shift, part in (
        (0, upper * (1.0 - east)),
        (1, lower * (1.0 - east)),
        (step, upper * east),
        (step + 1, lower * east),
    ):
        high = part.astype(BF16).astype(F32)
        corners.append((first + shift, high, part - high))

    def wide(values, slot, count):
        tile = jnp.broadcast_to(values[slot : slot + 1], (16, width)).astype(BF16)
        return jnp.concatenate([tile] * (count // 16), axis=0)

    fine_axis = iota((fine, width), 0).astype(F32).astype(BF16)
    coarse_axis = (iota((coarse, width), 0) - coarse // 2).astype(F32).astype(BF16)
    zero = jnp.zeros((), BF16)
    one = jnp.ones((), BF16)
    left, right = [], []
    for slot in range(capacity):
        high = low = zero
        for place, top, rest in corners:
            hit = fine_axis == wide(place, slot, fine)
            high = jnp.where(hit, wide(top, slot, fine), high)
            low = jnp.where(hit, wide(rest, slot, fine), low)
        left.append(jnp.concatenate([high, low], axis=0))
        right.append(jnp.where(coarse_axis == wide(group, slot, coarse), one, zero))
    return lax.dot_general(
        jnp.concatenate(left, axis=1),
        jnp.concatenate(right, axis=1),
        (((1,), (1,)), ((), ())),
        preferred_element_type=F32,
    )


def kernel(
    capacity,
    innov_hbm, error_hbm, offset_hbm, cell_hbm, owner_hbm, count_ref, land_hbm, inertia_hbm, depth_hbm,
    x_ref, r_ref,
    innov_ref, error_ref, offset_ref, cell_ref, owner_ref, land_ref, depth_ref, ground_ref,
    sent_ref, inbox_ref, acc_ref, perm_ref,
    tile_ref, pack_ref, strip_ref, pair_ref, edge_ref, side_ref,
    up_ref, down_ref, mid_ref, cwest_ref, ceast_ref,
    ocean_ref, diag_ref, cn_ref, cs_ref, cw_ref, ce_ref, q_ref,
    part_ref, slot_ref, gram_ref,
    in_sem, send_sem, recv_sem, halo_send, halo_recv, swap_send, swap_recv, sum_send, sum_recv,
):
    n_lat, n_lon, n_obs = (lax.axis_size(name) for name in AXES)
    lat, lon, core = (lax.axis_index(name) for name in AXES)
    tiles = n_lat * n_lon
    total = tiles * n_obs
    me = (lat * n_lon + lon) * n_obs + core
    rows, cols = x_ref.shape
    tall = rows + 2 * ROW_PAD
    keep = rows + ROW_PAD
    tile_rows = rows * n_obs
    blocks, width = innov_ref.shape
    cap_pad = sent_ref.shape[1]
    fine = fine_size()
    coarse = acc_ref.shape[1]
    group_cols = cols // FINE_COL

    loads = [
        pltpu.make_async_copy(source, target, in_sem.at[number])
        for number, (source, target) in enumerate(
            (
                (owner_hbm, owner_ref),
                (innov_hbm, innov_ref),
                (error_hbm, error_ref),
                (offset_hbm, offset_ref),
                (cell_hbm, cell_ref),
                (land_hbm, land_ref),
                (depth_hbm, depth_ref),
                (inertia_hbm, ground_ref.at[1]),
            )
        )
    ]
    for load in loads:
        load.start()

    barrier = pltpu.get_barrier_semaphore()

    def hop_of(ring_step):
        odd = ring_step % 2
        hop = odd * ((ring_step + 1) // 2) + (1 - odd) * (n_lat - ring_step // 2)
        return hop % n_lat

    def everyone(act):
        def line_of(k, carry):
            to_lat = lax.rem(lat + hop_of(n_lat - k), n_lat)
            for shift in range(n_lon):
                to_lon = lax.rem(lon + shift, n_lon)
                for peer in range(n_obs):
                    act((to_lat, to_lon, peer))
            return carry

        lax.fori_loop(1, n_lat, line_of, 0)
        for shift in range(1, n_lon):
            to_lon = lax.rem(lon + shift, n_lon)
            for peer in range(n_obs):
                act((lat, to_lon, peer))
        act((lat, lon, 1 - core))

    everyone(lambda device: pl.semaphore_signal(barrier, inc=1, device_id=device, device_id_type=MESH))

    loads[0].wait()
    count = count_ref[0]
    owner_row = jnp.broadcast_to(owner_ref[...].astype(F32), (blocks, blocks))
    owner_col = owner_row.T
    earlier = (iota((blocks, blocks), 0) < iota((blocks, blocks), 1)) & (
        iota((blocks, blocks), 0) < count
    )
    same = jnp.where((owner_row == owner_col) & earlier, 1.0, 0.0)
    rank = jnp.sum(same, axis=0, keepdims=True)
    slot_of = owner_row[:1] * cap_pad + rank
    slot_of = jnp.where(iota((1, blocks), 1) < count, slot_of, -1.0)
    slots = tiles * cap_pad
    chosen = iota((slots, blocks), 0).astype(F32) == slot_of
    chosen = jnp.where(chosen, 1.0, 0.0).astype(BF16)
    for load in loads[1:5]:
        load.wait()
    error = error_ref[...]
    data = jnp.concatenate(
        [
            innov_ref[...] / (error * error),
            offset_ref[0],
            offset_ref[1],
            cell_ref[...].astype(F32),
        ],
        axis=1,
    )
    high = data.astype(BF16)
    rest = data - high.astype(F32)
    middle = rest.astype(BF16)
    low = (rest - middle.astype(F32)).astype(BF16)
    sent_ref[...] = jnp.dot(
        jnp.concatenate([chosen] * 3, axis=1),
        jnp.concatenate([high, middle, low], axis=0),
        preferred_element_type=F32,
    ).reshape(sent_ref.shape)
    for load in loads[5:]:
        load.wait()
    ground_ref[0] = land_ref[...].astype(F32) * depth_ref[...]
    def block_copy(k):
        hop, shift = hop_of(k // n_lon), k % n_lon
        to_lat, to_lon = (lat + hop) % n_lat, (lon + shift) % n_lon
        return pltpu.make_async_remote_copy(
            src_ref=sent_ref.at[to_lat * n_lon + to_lon],
            dst_ref=inbox_ref.at[k],
            send_sem=send_sem.at[k],
            recv_sem=recv_sem.at[k],
            device_id=(to_lat, to_lon, core),
            device_id_type=MESH,
        )

    def send(k, carry):
        block_copy(k).start()
        return carry

    def halo_copy(index, source, target, device):
        return pltpu.make_async_remote_copy(
            src_ref=source,
            dst_ref=target,
            send_sem=halo_send.at[index],
            recv_sem=halo_recv.at[index],
            device_id=device,
            device_id_type=MESH,
        )

    ring = n_lat * n_obs
    line = lat * n_obs + core
    above = lax.rem(line + ring - 1, ring)
    below = lax.rem(line + 1, ring)
    west = lax.rem(lon + n_lon - 1, n_lon)
    east = lax.rem(lon + 1, n_lon)
    to_below = halo_copy(
        0, ground_ref.at[:, pl.ds(rows - ROW_PAD, ROW_PAD)], up_ref, (below // n_obs, lon, below % n_obs)
    )
    to_above = halo_copy(
        1, ground_ref.at[:, pl.ds(0, ROW_PAD)], down_ref, (above // n_obs, lon, above % n_obs)
    )
    to_east = halo_copy(2, mid_ref.at[:, :, pl.ds(cols - COL_PAD, COL_PAD)], cwest_ref, (lat, east, core))
    to_west = halo_copy(3, mid_ref.at[:, :, pl.ds(0, COL_PAD)], ceast_ref, (lat, west, core))

    def post_sum(turn, parts):
        stack = jnp.concatenate(
            parts + [jnp.zeros((COL_PAD - 8 * len(parts), COL_PAD), F32)], axis=0
        )
        values = jnp.sum(stack.T, axis=0, keepdims=True)
        slot_ref[turn, pl.ds(me, 1)] = values[None]
        part_ref[turn] = values

        everyone(
            lambda device: pltpu.make_async_remote_copy(
                src_ref=part_ref.at[turn],
                dst_ref=slot_ref.at[turn, me],
                send_sem=sum_send.at[turn],
                recv_sem=sum_recv.at[turn],
                device_id=device,
                device_id_type=MESH,
            ).start()
        )

    def take_sum(turn, number):
        block = slot_ref.at[turn, pl.ds(0, total - 1)]
        pltpu.make_async_copy(block, block, sum_recv.at[turn]).wait()
        pltpu.make_async_copy(block, block, sum_send.at[turn]).wait()
        values = jnp.sum(slot_ref[turn], axis=0)
        gram_ref[...] = jnp.broadcast_to(values, (COL_PAD, COL_PAD)).T
        return [
            jnp.sum(gram_ref[8 * k : 8 * k + 8], axis=0, keepdims=True) for k in range(number)
        ]

    def inner(value):
        return value[ROW_PAD:keep, :cols]

    def fold(value):
        out = value[:8]
        for start in range(8, rows, 8):
            out = out + value[start : start + 8]
        lanes = out[:, :COL_PAD]
        for start in range(COL_PAD, cols, COL_PAD):
            lanes = lanes + out[:, start : start + COL_PAD]
        return lanes

    def spread(k):
        return spread_block(capacity, width, cols, coarse, k)

    acc_ref[...] = spread(sent_ref[lat * n_lon + lon])

    def fill(part, carry):
        shape = (group_cols, cols)
        target = iota(shape, 0) * FINE_COL + part
        start = pl.multiple_of(part * group_cols, group_cols)
        perm_ref[pl.ds(start, group_cols)] = jnp.where(target == iota(shape, 1), 1.0, 0.0).astype(BF16)
        return carry

    lax.fori_loop(0, FINE_COL, fill, 0)
    pl.semaphore_wait(barrier, total - 1)
    to_below.start()
    to_above.start()
    lax.fori_loop(1, tiles, send, 0)

    def turn(k, carry):
        block_copy(k).wait_recv()
        acc_ref[...] = acc_ref[...] + spread(inbox_ref[k])

        @pl.when(k == tiles // 4 - 1)
        def _():
            to_below.wait()
            to_above.wait()
            mid_ref[:, :ROW_PAD] = up_ref[...]
            mid_ref[:, ROW_PAD:keep] = ground_ref[...]
            mid_ref[:, keep:] = down_ref[...]
            to_east.start()
            to_west.start()

        @pl.when(k == 3 * tiles // 4 - 1)
        def _():
            to_east.wait()
            to_west.wait()
            near = iota((tall, COL_PAD), 1) < COL_PAD // 2

            def widened(index):
                pad = jnp.where(near, ceast_ref[index], cwest_ref[index])
                return jnp.concatenate([mid_ref[index], pad], axis=1)

            conduct = widened(0)
            cn = jnp.sqrt(conduct * moved(conduct, 0, False))
            cs = moved(cn, 0, True)
            cw = jnp.sqrt(conduct * moved(conduct, 1, False))
            ce = moved(cw, 1, True)
            ocean = jnp.where(conduct > 0.0, 1.0, 0.0)
            diag = widened(1) + cn + cs + cw + ce
            cn_ref[...] = cn
            cs_ref[...] = cs
            cw_ref[...] = cw
            ce_ref[...] = ce
            ocean_ref[...] = ocean
            diag_ref[...] = diag
            kept = inner(diag) * inner(ocean)
            faces = cn * cn + cs * cs + cw * cw + ce * ce
            post_sum(0, [fold(inner(ocean)), fold(kept), fold(kept * kept), fold(inner(faces))])

        return carry

    lax.fori_loop(1, tiles, turn, 0)

    acc_ref[:fine] = acc_ref[:fine] + acc_ref[fine:]
    step = FINE_ROW + 1
    top_row = iota((8, group_cols), 0) == 0
    blank = jnp.zeros((FINE_ROW - 8, group_cols), F32)
    planes = []
    for part in range(FINE_COL + 1):
        pieces, spill = [], None
        for index in range(tile_rows // FINE_ROW):
            lanes = slice(index * group_cols, (index + 1) * group_cols)
            piece = acc_ref[part * step : part * step + FINE_ROW, lanes]
            if spill is not None:
                piece = piece + jnp.concatenate([spill, blank], axis=0)
            pieces.append(piece)
            last = acc_ref[part * step + FINE_ROW : part * step + step, lanes]
            spill = jnp.where(top_row, last, 0.0)
        planes.append(jnp.concatenate(pieces + [spill], axis=0))
    over = pltpu.roll(planes[FINE_COL], 1, 1)
    lane = iota(over.shape, 1)
    planes[0] = planes[0] + jnp.where(lane > 0, over, 0.0)
    beyond = jnp.where(lane == 0, over, 0.0)
    mixed = jnp.concatenate(planes[:FINE_COL], axis=1)
    high = mixed.astype(BF16).astype(F32)
    mixed = jnp.concatenate([high, mixed - high], axis=0).astype(BF16)
    natural = jnp.dot(mixed, perm_ref[...], preferred_element_type=F32)
    tile_tall = tile_rows + ROW_PAD
    natural = natural[:tile_tall] + natural[tile_tall:]
    tile_ref[:, :cols] = natural
    tile_ref[:, cols:] = beyond
    top = iota((ROW_PAD, cols + COL_PAD), 0) == 0
    pack_ref[...] = jnp.where(
        top, tile_ref[tile_rows:], tile_ref[tile_rows - ROW_PAD : tile_rows]
    )
    sides = jnp.where(lane < COL_PAD // 2, natural[:, :COL_PAD], natural[:, cols - COL_PAD :])
    sides = jnp.where(lane == COL_PAD - 8, pltpu.roll(beyond, COL_PAD - 8, 1), sides)
    sides = jnp.concatenate([sides, jnp.zeros((COL_PAD - tile_tall, COL_PAD), F32)], axis=0)
    strip_ref[...] = sides.T

    split = rows - ROW_PAD
    mine = pl.multiple_of(core * split, 8)
    theirs = pl.multiple_of((1 - core) * split, 8)
    north = lat > 0
    south = lat < n_lat - 1
    from_west = strip_ref.at[pl.ds(0, 8)]
    from_east = strip_ref.at[pl.ds(COL_PAD - 8, 8)]

    def swap_copy(out, into, source, target, device):
        return pltpu.make_async_remote_copy(
            src_ref=source,
            dst_ref=target,
            send_sem=swap_send.at[out],
            recv_sem=swap_recv.at[into],
            device_id=device,
            device_id_type=MESH,
        )

    up_lat, down_lat = jnp.maximum(lat - 1, 0), jnp.minimum(lat + 1, n_lat - 1)

    def northern():
        return [
            swap_copy(1, 1 + core, tile_ref.at[pl.ds(0, 8)], edge_ref.at[core], (up_lat, lon, 1)),
            swap_copy(2, 3 + core, from_west, side_ref.at[2 + core], (up_lat, west, 1)),
            swap_copy(3, 5 + core, from_east, side_ref.at[6 + core], (up_lat, east, 1)),
        ]

    def southern():
        return [
            swap_copy(4, 1 + core, pack_ref, edge_ref.at[core], (down_lat, lon, 0)),
            swap_copy(5, 3 + core, from_west, side_ref.at[2 + core], (down_lat, west, 0)),
            swap_copy(6, 5 + core, from_east, side_ref.at[6 + core], (down_lat, east, 0)),
        ]

    level = [
        swap_copy(7 + peer, 7 + core, from_west, side_ref.at[core], (lat, west, peer))
        for peer in range(2)
    ] + [
        swap_copy(9 + peer, 9 + core, from_east, side_ref.at[4 + core], (lat, east, peer))
        for peer in range(2)
    ]
    swap = swap_copy(0, 0, tile_ref.at[pl.ds(theirs, tall)], pair_ref, (lat, lon, 1 - core))

    @pl.when(north)
    def _():
        for item in northern():
            item.start()

    @pl.when(south)
    def _():
        for item in southern():
            item.start()

    for item in level:
        item.start()
    swap.start()

    linked = jnp.where(core == 0, lat, n_lat - 1 - lat) > 0

    def arrived(number, target):
        return swap_copy(0, number, target, target, (lat, lon, 1 - core))

    @pl.when(linked)
    def _():
        for sender in range(2):
            arrived(1 + sender, edge_ref.at[sender]).wait_recv()
            arrived(3 + sender, side_ref.at[2 + sender]).wait_recv()
            arrived(5 + sender, side_ref.at[6 + sender]).wait_recv()

    @pl.when(jnp.logical_not(linked))
    def _():
        edge_ref[...] = jnp.zeros_like(edge_ref)
        side_ref[2:4] = jnp.zeros((2, 8, COL_PAD), F32)
        side_ref[6:8] = jnp.zeros((2, 8, COL_PAD), F32)

    for sender in range(2):
        arrived(7 + sender, side_ref.at[sender]).wait_recv()
        arrived(9 + sender, side_ref.at[4 + sender]).wait_recv()

    def aligned(straight, corner):
        first = core == 0
        straight = jnp.where(
            first, pltpu.roll(straight, ROW_PAD, 1), pltpu.roll(straight, COL_PAD - split, 1)
        )
        corner = jnp.where(
            first,
            pltpu.roll(corner, COL_PAD - (tile_rows - ROW_PAD), 1),
            pltpu.roll(corner, keep, 1),
        )
        return straight + corner

    right_side = aligned(side_ref[0] + side_ref[1], side_ref[2] + side_ref[3])
    left_side = aligned(side_ref[4] + side_ref[5], side_ref[6] + side_ref[7])
    hole = jnp.zeros((COL_PAD - 16, COL_PAD), F32)
    beside = jnp.concatenate([right_side, hole, left_side], axis=0).T[:tall]
    entering = jnp.where(iota(beside.shape, 1) == 0, pltpu.roll(beside, 8, 1), 0.0)
    edge = edge_ref[0] + edge_ref[1]
    swap.wait_recv()

    @pl.when(core == 0)
    def _():
        q_ref[0, :ROW_PAD] = jnp.where(top, 0.0, edge)
        q_ref[0, ROW_PAD : 2 * ROW_PAD] = (
            tile_ref[:ROW_PAD] + pair_ref[:ROW_PAD] + jnp.where(top, edge, 0.0)
        )
        q_ref[0, 2 * ROW_PAD :] = tile_ref[ROW_PAD:keep] + pair_ref[ROW_PAD:keep]

    @pl.when(core == 1)
    def _():
        q_ref[0, :keep] = tile_ref[pl.ds(split, keep)] + pair_ref[:keep]
        q_ref[0, keep:] = tile_ref[pl.ds(split + keep, ROW_PAD)] + pair_ref[keep:] + edge

    q_ref[0, :, :COL_PAD] = q_ref[0, :, :COL_PAD] + entering
    q_ref[0, :, cols:] = q_ref[0, :, cols:] + beside
    q_ref[0] = q_ref[0] * ocean_ref[...]

    ocean_count, diag_sum, diag_square, face_square = take_sum(0, 4)
    ocean_count = jnp.maximum(ocean_count, 1.0)
    mean = diag_sum / ocean_count
    spread_out = jnp.maximum((diag_square + face_square) / ocean_count - mean * mean, 0.0)
    mean = 1.2 * mean

    def across(value, size):
        return jnp.concatenate([value] * (size // COL_PAD), axis=1)

    diag_ref[...] = diag_ref[...] - across(mean, cols + COL_PAD)

    spread_wide = across(spread_out, cols + COL_PAD)
    for k in range(ITERS):
        field = q_ref[k]
        value = (
            diag_ref[...] * field
            - cn_ref[...] * moved(field, 0, False)
            - cs_ref[...] * moved(field, 0, True)
            - cw_ref[...] * moved(field, 1, False)
            - ce_ref[...] * moved(field, 1, True)
        )
        if k:
            value = value - spread_wide * q_ref[k - 1]
        q_ref[k + 1] = value

    fields = [q_ref[k, ROW_PAD:keep, :cols] for k in range(ITERS + 1)]
    pairs = [(k, k + d) for k in range(ITERS) for d in range(2)]
    post_sum(1, [fold(fields[i] * fields[j]) for i, j in pairs])
    sums = take_sum(1, len(pairs))
    gram = {}
    for (i, j), value in zip(pairs, sums):
        gram[i, j] = gram[j, i] = value
    for gap in range(1, ITERS):
        for i in range(ITERS - gap):
            j = i + gap
            value = gram[i + 1, j]
            if i:
                value = value + spread_out * (gram[i - 1, j] - gram[i, j - 1])
            else:
                value = value - spread_out * gram[i, j - 1]
            gram[i, j + 1] = gram[j + 1, i] = value

    def plus(one, two):
        if one is None or two is None:
            return two if one is None else one
        return one + two

    def times(weight, part):
        return None if part is None else weight * part

    def quad(first, second):
        out = None
        for i, one in enumerate(first):
            line = None
            for j, two in enumerate(second):
                if one is not None and two is not None:
                    line = plus(line, two * gram[i, j])
            out = plus(out, times(one, line) if one is not None else None)
        return out

    def apply(weights):
        out = [None] * (ITERS + 1)
        for k, weight in enumerate(weights[:ITERS]):
            if weight is not None:
                out[k + 1] = plus(out[k + 1], weight)
                out[k] = plus(out[k], mean * weight)
                if k:
                    out[k - 1] = plus(out[k - 1], spread_out * weight)
        return out

    unit = jnp.ones((1, COL_PAD), F32)
    direct = [unit] + [None] * ITERS
    resid = [unit] + [None] * ITERS
    gained = [None] * (ITERS + 1)
    norm = gram[0, 0]
    for done in range(1, ITERS + 1):
        applied = apply(direct)
        step_size = norm / quad(direct, applied)
        gained = [plus(one, times(step_size, two)) for one, two in zip(gained, direct)]
        resid = [plus(one, times(-step_size, two)) for one, two in zip(resid, applied)]
        if done < ITERS:
            norm_next = quad(resid, resid)
            ratio = norm_next / norm
            direct = [plus(one, times(ratio, two)) for one, two in zip(resid, direct)]
            norm = norm_next

    def mix(weights):
        out = None
        for k, weight in enumerate(weights):
            if weight is not None:
                out = plus(out, across(weight, cols) * q_ref[k, ROW_PAD:keep, :cols])
        return out

    x_ref[...] = mix(gained)
    r_ref[...] = mix(resid)

    def finish(k, carry):
        block_copy(k).wait_send()
        return carry

    lax.fori_loop(1, tiles, finish, 0)
    swap.wait_send()
    for item in level:
        item.wait_send()

    @pl.when(north)
    def _():
        for item in northern():
            item.wait_send()

    @pl.when(south)
    def _():
        for item in southern():
            item.wait_send()


def body(
    innovation, obs_error, obs_offset, obs_cell, obs_owner, block_count,
    land_mask, inertia, sea_depth,
):
    block_total = obs_owner.shape[1]
    width = innovation.shape[1]
    n_lat, n_lon, n_obs = (lax.axis_size(name) for name in AXES)
    tiles = n_lat * n_lon
    capacity = max(3, 2 * ((block_total + tiles - 1) // tiles))
    cap_pad = -(-capacity // 8) * 8
    rows, cols = land_mask.shape
    total = tiles * n_obs
    coarse = (rows * n_obs // FINE_ROW) * (cols // FINE_COL)
    tall, broad = rows + 2 * ROW_PAD, cols + COL_PAD
    tile_tall = rows * n_obs + ROW_PAD
    vmem = lambda *shape: pltpu.VMEM(shape, F32)
    whole = pl.BlockSpec(memory_space=pltpu.VMEM)
    far = pl.BlockSpec(memory_space=pltpu.HBM)
    near = pl.BlockSpec(memory_space=pltpu.SMEM)
    dma = pltpu.SemaphoreType.DMA
    return pl.pallas_call(
        functools.partial(kernel, capacity),
        out_shape=[jax.ShapeDtypeStruct((rows, cols), F32)] * 2,
        in_specs=[far] * 5 + [near] + [far] * 3,
        out_specs=[whole] * 2,
        scratch_shapes=[
            vmem(*innovation.shape),
            vmem(*obs_error.shape),
            vmem(*obs_offset.shape),
            pltpu.VMEM(obs_cell.shape, jnp.int32),
            pltpu.VMEM(obs_owner.shape, jnp.int32),
            pltpu.VMEM((rows, cols), jnp.int32),
            vmem(rows, cols),
            vmem(2, rows, cols),
            vmem(tiles, cap_pad, 4 * width),
            vmem(tiles, cap_pad, 4 * width),
            vmem(2 * fine_size(), coarse),
            pltpu.VMEM((cols, cols), BF16),
            vmem(tile_tall, broad),
            vmem(ROW_PAD, broad),
            vmem(COL_PAD, COL_PAD),
            vmem(tall, broad),
            vmem(2, ROW_PAD, broad),
            vmem(8, 8, COL_PAD),
            vmem(2, ROW_PAD, cols),
            vmem(2, ROW_PAD, cols),
            vmem(2, tall, cols),
            vmem(2, tall, COL_PAD),
            vmem(2, tall, COL_PAD),
        ]
        + [vmem(tall, broad)] * 6
        + [
            vmem(ITERS + 1, tall, broad),
            vmem(2, 1, COL_PAD),
            vmem(2, total, 1, COL_PAD),
            vmem(COL_PAD, COL_PAD),
            dma((8,)),
            dma((tiles,)),
            dma((tiles,)),
            dma((4,)),
            dma((4,)),
            dma((11,)),
            dma((11,)),
            dma((2,)),
            dma((2,)),
        ],
        compiler_params=pltpu.CompilerParams(collective_id=0, has_side_effects=True),
        name="adjoint",
    )(
        innovation, obs_error, obs_offset, obs_cell, obs_owner, block_count,
        land_mask, inertia, sea_depth,
    )


def solution(mesh):
    spread = P(AXES, None)
    grid = P(("lat", "obs"), "lon")
    in_specs = (spread, spread, P(None, AXES, None), spread, spread, P(AXES), grid, grid, grid)
    return jax.shard_map(
        body, mesh=mesh, in_specs=in_specs, out_specs=(grid, grid), check_vma=False
    )
```

```python
import functools

import jax
import jax.numpy as jnp
from jax import lax
from jax.experimental import pallas as pl
from jax.experimental.pallas import tpu as pltpu
from jax.sharding import PartitionSpec as P

ITERS = 5
ROW_PAD = 8
COL_PAD = 128
FINE_ROW = 16
FINE_COL = 8
MESH = pl.DeviceIdType.MESH
AXES = ("lat", "lon", "obs")
F32 = jnp.float32
BF16 = jnp.bfloat16


def iota(shape, axis):
    return lax.broadcasted_iota(jnp.int32, shape, axis)


def moved(value, axis, back):
    size = value.shape[axis]
    return pltpu.roll(value, size - 1 if back else 1, axis)


def fine_size():
    return -(-(FINE_ROW + 1) * (FINE_COL + 1) // 16) * 16


def operands(capacity, width, cols, coarse, block):
    fine = fine_size()
    amount = block[:, :width]
    north = block[:, width : 2 * width]
    east = block[:, 2 * width : 3 * width]
    cell = block[:, 3 * width :]
    row = jnp.floor(cell * (1.0 / cols))
    col = cell - row * cols
    row_group = jnp.floor(row * (1.0 / FINE_ROW))
    col_group = jnp.floor(col * (1.0 / FINE_COL))
    step = FINE_ROW + 1
    first = (col - col_group * FINE_COL) * step + (row - row_group * FINE_ROW)
    group = row_group * (cols // FINE_COL) + col_group - coarse // 2
    upper = amount * (1.0 - north)
    lower = amount * north
    corners = []
    for shift, part in (
        (0, upper * (1.0 - east)),
        (1, lower * (1.0 - east)),
        (step, upper * east),
        (step + 1, lower * east),
    ):
        high = part.astype(BF16).astype(F32)
        corners.append((first + shift, high, part - high))

    def wide(values, slot, count):
        tile = jnp.broadcast_to(values[slot : slot + 1], (16, width)).astype(BF16)
        return jnp.concatenate([tile] * (count // 16), axis=0)

    fine_axis = iota((fine, width), 0).astype(F32).astype(BF16)
    coarse_axis = (iota((coarse, width), 0) - coarse // 2).astype(F32).astype(BF16)
    zero = jnp.zeros((), BF16)
    one = jnp.ones((), BF16)
    left, right = [], []
    for slot in range(capacity):
        high = low = zero
        for place, top, rest in corners:
            hit = fine_axis == wide(place, slot, fine)
            high = jnp.where(hit, wide(top, slot, fine), high)
            low = jnp.where(hit, wide(rest, slot, fine), low)
        left.append(jnp.concatenate([high, low], axis=0))
        right.append(jnp.where(coarse_axis == wide(group, slot, coarse), one, zero))
    return left, right


def spread_blocks(capacity, width, cols, coarse, blocks):
    left, right = [], []
    for block in blocks:
        more_left, more_right = operands(capacity, width, cols, coarse, block)
        left += more_left
        right += more_right
    return lax.dot_general(
        jnp.concatenate(left, axis=1),
        jnp.concatenate(right, axis=1),
        (((1,), (1,)), ((), ())),
        preferred_element_type=F32,
    )


def kernel(
    capacity,
    innov_hbm, error_hbm, offset_hbm, cell_hbm, owner_hbm, count_hbm, land_hbm, inertia_hbm, depth_hbm,
    x_ref, r_ref,
    innov_ref, error_ref, offset_ref, cell_ref, owner_ref, count_ref, land_ref, depth_ref, ground_ref,
    sent_ref, inbox_ref, acc_ref, perm_ref,
    tile_ref, pack_ref, strip_ref, pair_ref, edge_ref, side_ref,
    mid_ref, cwest_ref, ceast_ref,
    ocean_ref, diag_ref, cn_ref, cs_ref, cw_ref, ce_ref, q_ref,
    part_ref, slot_ref, gram_ref,
    in_sem, send_sem, recv_sem, halo_send, halo_recv, swap_send, swap_recv, sum_send, sum_recv,
):
    n_lat, n_lon, n_obs = (lax.axis_size(name) for name in AXES)
    lat, lon, core = (lax.axis_index(name) for name in AXES)
    tiles = n_lat * n_lon
    total = tiles * n_obs
    me = (lat * n_lon + lon) * n_obs + core
    rows, cols = x_ref.shape
    tall = rows + 2 * ROW_PAD
    keep = rows + ROW_PAD
    tile_rows = rows * n_obs
    blocks, width = innov_ref.shape
    cap_pad = sent_ref.shape[1]
    fine = fine_size()
    coarse = acc_ref.shape[1]
    group_cols = cols // FINE_COL

    loads = [
        pltpu.make_async_copy(source, target, in_sem.at[number])
        for number, (source, target) in enumerate(
            (
                (count_hbm, count_ref),
                (owner_hbm, owner_ref),
                (innov_hbm, innov_ref),
                (error_hbm, error_ref),
                (offset_hbm, offset_ref),
                (cell_hbm, cell_ref),
                (land_hbm, land_ref),
                (depth_hbm, depth_ref),
                (inertia_hbm, ground_ref.at[1]),
            )
        )
    ]
    for load in loads:
        load.start()

    barrier = pltpu.get_barrier_semaphore()

    def hop_of(ring_step):
        odd = ring_step % 2
        hop = odd * ((ring_step + 1) // 2) + (1 - odd) * (n_lat - ring_step // 2)
        return hop % n_lat

    def everyone(act):
        def line_of(k, carry):
            to_lat = lax.rem(lat + hop_of(n_lat - k), n_lat)
            for shift in range(n_lon):
                to_lon = lax.rem(lon + shift, n_lon)
                for peer in range(n_obs):
                    act((to_lat, to_lon, peer))
            return carry

        lax.fori_loop(1, n_lat, line_of, 0)
        for shift in range(1, n_lon):
            to_lon = lax.rem(lon + shift, n_lon)
            for peer in range(n_obs):
                act((lat, to_lon, peer))
        act((lat, lon, 1 - core))

    everyone(lambda device: pl.semaphore_signal(barrier, inc=1, device_id=device, device_id_type=MESH))

    for load in loads[:2]:
        load.wait()
    count = count_ref[0]
    owner_row = jnp.broadcast_to(owner_ref[...].astype(F32), (blocks, blocks))
    owner_col = owner_row.T
    earlier = (iota((blocks, blocks), 0) < iota((blocks, blocks), 1)) & (
        iota((blocks, blocks), 0) < count
    )
    same = jnp.where((owner_row == owner_col) & earlier, 1.0, 0.0)
    rank = jnp.sum(same, axis=0, keepdims=True)
    slot_of = owner_row[:1] * cap_pad + rank
    slot_of = jnp.where(iota((1, blocks), 1) < count, slot_of, -1.0)
    slots = tiles * cap_pad
    chosen = iota((slots, blocks), 0).astype(F32) == slot_of
    chosen = jnp.where(chosen, 1.0, 0.0).astype(BF16)
    for load in loads[2:6]:
        load.wait()
    error = error_ref[...]
    data = jnp.concatenate(
        [
            innov_ref[...] / (error * error),
            offset_ref[0],
            offset_ref[1],
            cell_ref[...].astype(F32),
        ],
        axis=1,
    )
    high = data.astype(BF16)
    rest = data - high.astype(F32)
    middle = rest.astype(BF16)
    low = (rest - middle.astype(F32)).astype(BF16)
    sent_ref[...] = jnp.dot(
        jnp.concatenate([chosen] * 3, axis=1),
        jnp.concatenate([high, middle, low], axis=0),
        preferred_element_type=F32,
    ).reshape(sent_ref.shape)
    for load in loads[6:]:
        load.wait()
    ground_ref[0] = land_ref[...].astype(F32) * depth_ref[...]
    def block_copy(k):
        hop, shift = hop_of(k // n_lon), k % n_lon
        to_lat, to_lon, bit = (lat + hop) % n_lat, 0, 1
        while bit < n_lon:
            to_lon = to_lon + bit * ((lon // bit + shift // bit) % 2)
            bit = 2 * bit
        return pltpu.make_async_remote_copy(
            src_ref=sent_ref.at[to_lat * n_lon + to_lon],
            dst_ref=inbox_ref.at[k],
            send_sem=send_sem.at[k],
            recv_sem=recv_sem.at[k],
            device_id=(to_lat, to_lon, core),
            device_id_type=MESH,
        )

    def send(k, carry):
        block_copy(k).start()
        return carry

    def halo_copy(index, source, target, device):
        return pltpu.make_async_remote_copy(
            src_ref=source,
            dst_ref=target,
            send_sem=halo_send.at[index],
            recv_sem=halo_recv.at[index],
            device_id=device,
            device_id_type=MESH,
        )

    line = lat * n_obs + core
    last_line = n_lat * n_obs - 1
    above = jnp.maximum(line - 1, 0)
    below = jnp.minimum(line + 1, last_line)
    above = (above // n_obs, above % n_obs)
    below = (below // n_obs, below % n_obs)
    west = lax.rem(lon + n_lon - 1, n_lon)
    east = lax.rem(lon + 1, n_lon)
    first_rows, last_rows = pl.ds(0, ROW_PAD), pl.ds(rows - ROW_PAD, ROW_PAD)
    first_cols, last_cols = pl.ds(0, COL_PAD), pl.ds(cols - COL_PAD, COL_PAD)
    row_before, row_after = pl.ds(0, ROW_PAD), pl.ds(keep, ROW_PAD)
    inside = pl.ds(ROW_PAD, rows)

    def across_lon(number, source_rows, target_rows, to_lat, to_core):
        return [
            halo_copy(
                number,
                ground_ref.at[:, source_rows, last_cols],
                cwest_ref.at[:, target_rows],
                (to_lat, east, to_core),
            ),
            halo_copy(
                number + 1,
                ground_ref.at[:, source_rows, first_cols],
                ceast_ref.at[:, target_rows],
                (to_lat, west, to_core),
            ),
        ]

    level_halo = across_lon(0, pl.ds(0, rows), inside, lat, core)

    def halo_above():
        to_lat, to_core = above
        return [
            halo_copy(2, ground_ref.at[:, first_rows], mid_ref.at[:, row_after], (to_lat, lon, to_core))
        ] + across_lon(3, first_rows, row_after, to_lat, to_core)

    def halo_below():
        to_lat, to_core = below
        return [
            halo_copy(5, ground_ref.at[:, last_rows], mid_ref.at[:, row_before], (to_lat, lon, to_core))
        ] + across_lon(6, last_rows, row_before, to_lat, to_core)

    def post_sum(turn, parts):
        stack = jnp.concatenate(
            parts + [jnp.zeros((COL_PAD - 8 * len(parts), COL_PAD), F32)], axis=0
        )
        values = jnp.sum(stack.T, axis=0, keepdims=True)
        slot_ref[turn, pl.ds(me, 1)] = values[None]
        part_ref[turn] = values

        everyone(
            lambda device: pltpu.make_async_remote_copy(
                src_ref=part_ref.at[turn],
                dst_ref=slot_ref.at[turn, me],
                send_sem=sum_send.at[turn],
                recv_sem=sum_recv.at[turn],
                device_id=device,
                device_id_type=MESH,
            ).start()
        )

    def take_sum(turn, number):
        block = slot_ref.at[turn, pl.ds(0, total - 1)]
        pltpu.make_async_copy(block, block, sum_recv.at[turn]).wait()
        pltpu.make_async_copy(block, block, sum_send.at[turn]).wait()
        values = jnp.sum(slot_ref[turn], axis=0)
        gram_ref[...] = jnp.broadcast_to(values, (COL_PAD, COL_PAD)).T
        return [
            jnp.sum(gram_ref[8 * k : 8 * k + 8], axis=0, keepdims=True) for k in range(number)
        ]

    def fold(value):
        out = value[:8]
        for start in range(8, rows, 8):
            out = out + value[start : start + 8]
        lanes = out[:, :COL_PAD]
        for start in range(COL_PAD, cols, COL_PAD):
            lanes = lanes + out[:, start : start + COL_PAD]
        return lanes

    def spread(*blocks):
        return spread_blocks(capacity, width, cols, coarse, blocks)

    pl.semaphore_wait(barrier, total - 1)
    lax.fori_loop(1, tiles, send, 0)
    for item in level_halo:
        item.start()

    @pl.when(line > 0)
    def _():
        for item in halo_above():
            item.start()

    @pl.when(line < last_line)
    def _():
        for item in halo_below():
            item.start()

    acc_ref[...] = spread(sent_ref[lat * n_lon + lon])

    def fill(part, carry):
        shape = (group_cols, cols)
        target = iota(shape, 0) * FINE_COL + part
        start = pl.multiple_of(part * group_cols, group_cols)
        perm_ref[pl.ds(start, group_cols)] = jnp.where(target == iota(shape, 1), 1.0, 0.0).astype(BF16)
        return carry

    lax.fori_loop(0, FINE_COL, fill, 0)

    conduct = ground_ref[0]
    kept = jnp.where(conduct > 0.0, 1.0, 0.0)
    row_face = conduct * moved(conduct, 0, False)
    col_face = conduct * moved(conduct, 1, False)
    faces = row_face + moved(row_face, 0, True) + col_face + moved(col_face, 1, True)
    row_face = jnp.sqrt(row_face)
    col_face = jnp.sqrt(col_face)
    center = ground_ref[1] + row_face + moved(row_face, 0, True) + col_face + moved(col_face, 1, True)
    center = center * kept
    post_sum(0, [fold(kept), fold(center), fold(center * center), fold(faces)])

    block_copy(1).wait_recv()
    acc_ref[...] = acc_ref[...] + spread(inbox_ref[1])

    def turn(k, carry):
        block_copy(2 * k).wait_recv()
        block_copy(2 * k + 1).wait_recv()
        acc_ref[...] = acc_ref[...] + spread(inbox_ref[2 * k], inbox_ref[2 * k + 1])
        return carry

    lax.fori_loop(1, tiles // 2, turn, 0)

    acc_ref[:fine] = acc_ref[:fine] + acc_ref[fine:]
    step = FINE_ROW + 1
    top_row = iota((8, group_cols), 0) == 0
    blank = jnp.zeros((FINE_ROW - 8, group_cols), F32)
    planes = []
    for part in range(FINE_COL + 1):
        pieces, spill = [], None
        for index in range(tile_rows // FINE_ROW):
            lanes = slice(index * group_cols, (index + 1) * group_cols)
            piece = acc_ref[part * step : part * step + FINE_ROW, lanes]
            if spill is not None:
                piece = piece + jnp.concatenate([spill, blank], axis=0)
            pieces.append(piece)
            last = acc_ref[part * step + FINE_ROW : part * step + step, lanes]
            spill = jnp.where(top_row, last, 0.0)
        planes.append(jnp.concatenate(pieces + [spill], axis=0))
    over = pltpu.roll(planes[FINE_COL], 1, 1)
    lane = iota(over.shape, 1)
    planes[0] = planes[0] + jnp.where(lane > 0, over, 0.0)
    beyond = jnp.where(lane == 0, over, 0.0)
    mixed = jnp.concatenate(planes[:FINE_COL], axis=1)
    high = mixed.astype(BF16).astype(F32)
    mixed = jnp.concatenate([high, mixed - high], axis=0).astype(BF16)
    natural = jnp.dot(mixed, perm_ref[...], preferred_element_type=F32)
    tile_tall = tile_rows + ROW_PAD
    natural = natural[:tile_tall] + natural[tile_tall:]
    tile_ref[:, :cols] = natural
    tile_ref[:, cols:] = beyond
    top = iota((ROW_PAD, cols + COL_PAD), 0) == 0
    pack_ref[...] = jnp.where(
        top, tile_ref[tile_rows:], tile_ref[tile_rows - ROW_PAD : tile_rows]
    )
    sides = jnp.where(lane < COL_PAD // 2, natural[:, :COL_PAD], natural[:, cols - COL_PAD :])
    sides = jnp.where(lane == COL_PAD - 8, pltpu.roll(beyond, COL_PAD - 8, 1), sides)
    sides = jnp.concatenate([sides, jnp.zeros((COL_PAD - tile_tall, COL_PAD), F32)], axis=0)
    strip_ref[...] = sides.T

    split = rows - ROW_PAD
    mine = pl.multiple_of(core * split, 8)
    theirs = pl.multiple_of((1 - core) * split, 8)
    north = lat > 0
    south = lat < n_lat - 1
    from_west = strip_ref.at[pl.ds(0, 8)]
    from_east = strip_ref.at[pl.ds(COL_PAD - 8, 8)]

    def swap_copy(out, into, source, target, device):
        return pltpu.make_async_remote_copy(
            src_ref=source,
            dst_ref=target,
            send_sem=swap_send.at[out],
            recv_sem=swap_recv.at[into],
            device_id=device,
            device_id_type=MESH,
        )

    up_lat, down_lat = jnp.maximum(lat - 1, 0), jnp.minimum(lat + 1, n_lat - 1)

    def northern():
        return [
            swap_copy(1, 1 + core, tile_ref.at[pl.ds(0, 8)], edge_ref.at[core], (up_lat, lon, 1)),
            swap_copy(2, 3 + core, from_west, side_ref.at[2 + core], (up_lat, west, 1)),
            swap_copy(3, 5 + core, from_east, side_ref.at[6 + core], (up_lat, east, 1)),
        ]

    def southern():
        return [
            swap_copy(4, 1 + core, pack_ref, edge_ref.at[core], (down_lat, lon, 0)),
            swap_copy(5, 3 + core, from_west, side_ref.at[2 + core], (down_lat, west, 0)),
            swap_copy(6, 5 + core, from_east, side_ref.at[6 + core], (down_lat, east, 0)),
        ]

    level = [
        swap_copy(7 + peer, 7 + core, from_west, side_ref.at[core], (lat, west, peer))
        for peer in range(2)
    ] + [
        swap_copy(9 + peer, 9 + core, from_east, side_ref.at[4 + core], (lat, east, peer))
        for peer in range(2)
    ]
    swap = swap_copy(0, 0, tile_ref.at[pl.ds(theirs, tall)], pair_ref, (lat, lon, 1 - core))

    @pl.when(north)
    def _():
        for item in northern():
            item.start()

    @pl.when(south)
    def _():
        for item in southern():
            item.start()

    for item in level:
        item.start()
    swap.start()

    mid_ref[:, inside] = ground_ref[...]

    @pl.when(line > 0)
    def _():
        for item in halo_below():
            item.wait_recv()

    @pl.when(line < last_line)
    def _():
        for item in halo_above():
            item.wait_recv()

    @pl.when(line == 0)
    def _():
        for ref in (mid_ref, cwest_ref, ceast_ref):
            ref[:, row_before] = jnp.zeros_like(ref[:, row_before])

    @pl.when(line == last_line)
    def _():
        for ref in (mid_ref, cwest_ref, ceast_ref):
            ref[:, row_after] = jnp.zeros_like(ref[:, row_after])

    for item in level_halo:
        item.wait_recv()
    near = iota((tall, COL_PAD), 1) < COL_PAD // 2

    def widened(index):
        pad = jnp.where(near, ceast_ref[index], cwest_ref[index])
        return jnp.concatenate([mid_ref[index], pad], axis=1)

    conduct = widened(0)
    cn = jnp.sqrt(conduct * moved(conduct, 0, False))
    cs = moved(cn, 0, True)
    cw = jnp.sqrt(conduct * moved(conduct, 1, False))
    ce = moved(cw, 1, True)
    cn_ref[...] = cn
    cs_ref[...] = cs
    cw_ref[...] = cw
    ce_ref[...] = ce
    ocean_ref[...] = jnp.where(conduct > 0.0, 1.0, 0.0)
    diag_ref[...] = widened(1) + cn + cs + cw + ce

    linked = jnp.where(core == 0, lat, n_lat - 1 - lat) > 0

    def arrived(number, target):
        return swap_copy(0, number, target, target, (lat, lon, 1 - core))

    @pl.when(linked)
    def _():
        for sender in range(2):
            arrived(1 + sender, edge_ref.at[sender]).wait_recv()
            arrived(3 + sender, side_ref.at[2 + sender]).wait_recv()
            arrived(5 + sender, side_ref.at[6 + sender]).wait_recv()

    @pl.when(jnp.logical_not(linked))
    def _():
        edge_ref[...] = jnp.zeros_like(edge_ref)
        side_ref[2:4] = jnp.zeros((2, 8, COL_PAD), F32)
        side_ref[6:8] = jnp.zeros((2, 8, COL_PAD), F32)

    for sender in range(2):
        arrived(7 + sender, side_ref.at[sender]).wait_recv()
        arrived(9 + sender, side_ref.at[4 + sender]).wait_recv()

    def aligned(straight, corner):
        first = core == 0
        straight = jnp.where(
            first, pltpu.roll(straight, ROW_PAD, 1), pltpu.roll(straight, COL_PAD - split, 1)
        )
        corner = jnp.where(
            first,
            pltpu.roll(corner, COL_PAD - (tile_rows - ROW_PAD), 1),
            pltpu.roll(corner, keep, 1),
        )
        return straight + corner

    right_side = aligned(side_ref[0] + side_ref[1], side_ref[2] + side_ref[3])
    left_side = aligned(side_ref[4] + side_ref[5], side_ref[6] + side_ref[7])
    hole = jnp.zeros((COL_PAD - 16, COL_PAD), F32)
    beside = jnp.concatenate([right_side, hole, left_side], axis=0).T[:tall]
    entering = jnp.where(iota(beside.shape, 1) == 0, pltpu.roll(beside, 8, 1), 0.0)
    edge = edge_ref[0] + edge_ref[1]
    swap.wait_recv()

    @pl.when(core == 0)
    def _():
        q_ref[0, :ROW_PAD] = jnp.where(top, 0.0, edge)
        q_ref[0, ROW_PAD : 2 * ROW_PAD] = (
            tile_ref[:ROW_PAD] + pair_ref[:ROW_PAD] + jnp.where(top, edge, 0.0)
        )
        q_ref[0, 2 * ROW_PAD :] = tile_ref[ROW_PAD:keep] + pair_ref[ROW_PAD:keep]

    @pl.when(core == 1)
    def _():
        q_ref[0, :keep] = tile_ref[pl.ds(split, keep)] + pair_ref[:keep]
        q_ref[0, keep:] = tile_ref[pl.ds(split + keep, ROW_PAD)] + pair_ref[keep:] + edge

    q_ref[0, :, :COL_PAD] = q_ref[0, :, :COL_PAD] + entering
    q_ref[0, :, cols:] = q_ref[0, :, cols:] + beside
    q_ref[0] = q_ref[0] * ocean_ref[...]

    ocean_count, diag_sum, diag_square, face_square = take_sum(0, 4)
    ocean_count = jnp.maximum(ocean_count, 1.0)
    mean = diag_sum / ocean_count
    spread_out = jnp.maximum((diag_square + face_square) / ocean_count - mean * mean, 0.0)
    mean = 1.2 * mean

    def across(value, size):
        return jnp.concatenate([value] * (size // COL_PAD), axis=1)

    diag_ref[...] = diag_ref[...] - across(mean, cols + COL_PAD)

    spread_wide = across(spread_out, cols + COL_PAD)
    for k in range(ITERS):
        field = q_ref[k]
        value = (
            diag_ref[...] * field
            - cn_ref[...] * moved(field, 0, False)
            - cs_ref[...] * moved(field, 0, True)
            - cw_ref[...] * moved(field, 1, False)
            - ce_ref[...] * moved(field, 1, True)
        )
        if k:
            value = value - spread_wide * q_ref[k - 1]
        q_ref[k + 1] = value

    fields = [q_ref[k, ROW_PAD:keep, :cols] for k in range(ITERS + 1)]
    pairs = [(k, k + d) for k in range(ITERS) for d in range(2)]
    post_sum(1, [fold(fields[i] * fields[j]) for i, j in pairs])
    sums = take_sum(1, len(pairs))
    gram = {}
    for (i, j), value in zip(pairs, sums):
        gram[i, j] = gram[j, i] = value
    for gap in range(1, ITERS):
        for i in range(ITERS - gap):
            j = i + gap
            value = gram[i + 1, j]
            if i:
                value = value + spread_out * (gram[i - 1, j] - gram[i, j - 1])
            else:
                value = value - spread_out * gram[i, j - 1]
            gram[i, j + 1] = gram[j + 1, i] = value

    def plus(one, two):
        if one is None or two is None:
            return two if one is None else one
        return one + two

    def times(weight, part):
        return None if part is None else weight * part

    def quad(first, second):
        out = None
        for i, one in enumerate(first):
            line = None
            for j, two in enumerate(second):
                if one is not None and two is not None:
                    line = plus(line, two * gram[i, j])
            out = plus(out, times(one, line) if one is not None else None)
        return out

    def apply(weights):
        out = [None] * (ITERS + 1)
        for k, weight in enumerate(weights[:ITERS]):
            if weight is not None:
                out[k + 1] = plus(out[k + 1], weight)
                out[k] = plus(out[k], mean * weight)
                if k:
                    out[k - 1] = plus(out[k - 1], spread_out * weight)
        return out

    unit = jnp.ones((1, COL_PAD), F32)
    direct = [unit] + [None] * ITERS
    resid = [unit] + [None] * ITERS
    gained = [None] * (ITERS + 1)
    norm = gram[0, 0]
    for done in range(1, ITERS + 1):
        applied = apply(direct)
        step_size = norm / quad(direct, applied)
        gained = [plus(one, times(step_size, two)) for one, two in zip(gained, direct)]
        resid = [plus(one, times(-step_size, two)) for one, two in zip(resid, applied)]
        if done < ITERS:
            norm_next = quad(resid, resid)
            ratio = norm_next / norm
            direct = [plus(one, times(ratio, two)) for one, two in zip(resid, direct)]
            norm = norm_next

    def mix(weights):
        out = None
        for k, weight in enumerate(weights):
            if weight is not None:
                out = plus(out, across(weight, cols) * q_ref[k, ROW_PAD:keep, :cols])
        return out

    x_ref[...] = mix(gained)
    r_ref[...] = mix(resid)

    def finish(k, carry):
        block_copy(k).wait_send()
        return carry

    lax.fori_loop(1, tiles, finish, 0)
    swap.wait_send()
    for item in level + level_halo:
        item.wait_send()

    @pl.when(line > 0)
    def _():
        for item in halo_above():
            item.wait_send()

    @pl.when(line < last_line)
    def _():
        for item in halo_below():
            item.wait_send()

    @pl.when(north)
    def _():
        for item in northern():
            item.wait_send()

    @pl.when(south)
    def _():
        for item in southern():
            item.wait_send()


def write(x_ref, r_ref, x_hbm, r_hbm, sem):
    copies = [
        pltpu.make_async_copy(x_ref, x_hbm, sem.at[0]),
        pltpu.make_async_copy(r_ref, r_hbm, sem.at[1]),
    ]
    for copy in copies:
        copy.start()
    for copy in copies:
        copy.wait()


def body(
    innovation, obs_error, obs_offset, obs_cell, obs_owner, block_count,
    land_mask, inertia, sea_depth,
):
    block_total = obs_owner.shape[1]
    width = innovation.shape[1]
    n_lat, n_lon, n_obs = (lax.axis_size(name) for name in AXES)
    tiles = n_lat * n_lon
    capacity = max(3, 2 * ((block_total + tiles - 1) // tiles))
    cap_pad = -(-capacity // 8) * 8
    rows, cols = land_mask.shape
    total = tiles * n_obs
    coarse = (rows * n_obs // FINE_ROW) * (cols // FINE_COL)
    tall, broad = rows + 2 * ROW_PAD, cols + COL_PAD
    tile_tall = rows * n_obs + ROW_PAD
    vmem = lambda *shape: pltpu.VMEM(shape, F32)
    whole = pl.BlockSpec(memory_space=pltpu.VMEM)
    far = pl.BlockSpec(memory_space=pltpu.HBM)
    dma = pltpu.SemaphoreType.DMA
    fields = pl.pallas_call(
        functools.partial(kernel, capacity),
        out_shape=[pltpu.VMEM((rows, cols), F32)] * 2,
        in_specs=[far] * 9,
        out_specs=[whole] * 2,
        scratch_shapes=[
            vmem(*innovation.shape),
            vmem(*obs_error.shape),
            vmem(*obs_offset.shape),
            pltpu.VMEM(obs_cell.shape, jnp.int32),
            pltpu.VMEM(obs_owner.shape, jnp.int32),
            pltpu.SMEM(block_count.shape, jnp.int32),
            pltpu.VMEM((rows, cols), jnp.int32),
            vmem(rows, cols),
            vmem(2, rows, cols),
            vmem(tiles, cap_pad, 4 * width),
            vmem(tiles, cap_pad, 4 * width),
            vmem(2 * fine_size(), coarse),
            pltpu.VMEM((cols, cols), BF16),
            vmem(tile_tall, broad),
            vmem(ROW_PAD, broad),
            vmem(COL_PAD, COL_PAD),
            vmem(tall, broad),
            vmem(2, ROW_PAD, broad),
            vmem(8, 8, COL_PAD),
            vmem(2, tall, cols),
            vmem(2, tall, COL_PAD),
            vmem(2, tall, COL_PAD),
        ]
        + [vmem(tall, broad)] * 6
        + [
            vmem(ITERS + 1, tall, broad),
            vmem(2, 1, COL_PAD),
            vmem(2, total, 1, COL_PAD),
            vmem(COL_PAD, COL_PAD),
            dma((9,)),
            dma((tiles,)),
            dma((tiles,)),
            dma((8,)),
            dma((8,)),
            dma((11,)),
            dma((11,)),
            dma((2,)),
            dma((2,)),
        ],
        compiler_params=pltpu.CompilerParams(collective_id=0, has_side_effects=True),
        name="adjoint",
    )(
        innovation, obs_error, obs_offset, obs_cell, obs_owner, block_count,
        land_mask, inertia, sea_depth,
    )
    return pl.pallas_call(
        write,
        out_shape=[jax.ShapeDtypeStruct((rows, cols), F32)] * 2,
        in_specs=[whole] * 2,
        out_specs=[far] * 2,
        scratch_shapes=[dma((2,))],
        name="write",
    )(*[pltpu.with_memory_space_constraint(field, pltpu.VMEM) for field in fields])


def solution(mesh):
    spread = P(AXES, None)
    grid = P(("lat", "obs"), "lon")
    in_specs = (spread, spread, P(None, AXES, None), spread, spread, P(AXES), grid, grid, grid)
    return jax.shard_map(
        body, mesh=mesh, in_specs=in_specs, out_specs=(grid, grid), check_vma=False
    )
```

```python
import functools

import jax
import jax.numpy as jnp
from jax import lax
from jax.experimental import pallas as pl
from jax.experimental.pallas import tpu as pltpu
from jax.sharding import PartitionSpec as P

ITERS = 5
ROW_PAD = 8
COL_PAD = 128
FINE_ROW = 16
FINE_COL = 8
MESH = pl.DeviceIdType.MESH
AXES = ("lat", "lon", "obs")
F32 = jnp.float32
BF16 = jnp.bfloat16


def iota(shape, axis):
    return lax.broadcasted_iota(jnp.int32, shape, axis)


def moved(value, axis, back):
    size = value.shape[axis]
    return pltpu.roll(value, size - 1 if back else 1, axis)


def fine_size():
    return -(-(FINE_ROW + 1) * (FINE_COL + 1) // 16) * 16


def operands(capacity, width, cols, coarse, block):
    fine = fine_size()
    amount = block[:, :width]
    north = block[:, width : 2 * width]
    east = block[:, 2 * width : 3 * width]
    cell = block[:, 3 * width :]
    row = jnp.floor(cell * (1.0 / cols))
    col = cell - row * cols
    row_group = jnp.floor(row * (1.0 / FINE_ROW))
    col_group = jnp.floor(col * (1.0 / FINE_COL))
    step = FINE_ROW + 1
    first = (col - col_group * FINE_COL) * step + (row - row_group * FINE_ROW)
    group = row_group * (cols // FINE_COL) + col_group - coarse // 2
    upper = amount * (1.0 - north)
    lower = amount * north
    corners = []
    for shift, part in (
        (0, upper * (1.0 - east)),
        (1, lower * (1.0 - east)),
        (step, upper * east),
        (step + 1, lower * east),
    ):
        high = part.astype(BF16).astype(F32)
        corners.append((first + shift, high, part - high))

    def wide(values, slot, count):
        tile = jnp.broadcast_to(values[slot : slot + 1], (16, width)).astype(BF16)
        return jnp.concatenate([tile] * (count // 16), axis=0)

    fine_axis = iota((fine, width), 0).astype(F32).astype(BF16)
    coarse_axis = (iota((coarse, width), 0) - coarse // 2).astype(F32).astype(BF16)
    zero = jnp.zeros((), BF16)
    one = jnp.ones((), BF16)
    left, right = [], []
    for slot in range(capacity):
        high = low = zero
        for place, top, rest in corners:
            hit = fine_axis == wide(place, slot, fine)
            high = jnp.where(hit, wide(top, slot, fine), high)
            low = jnp.where(hit, wide(rest, slot, fine), low)
        left.append(jnp.concatenate([high, low], axis=0))
        right.append(jnp.where(coarse_axis == wide(group, slot, coarse), one, zero))
    return left, right


def spread_blocks(capacity, width, cols, coarse, blocks):
    left, right = [], []
    for block in blocks:
        more_left, more_right = operands(capacity, width, cols, coarse, block)
        left += more_left
        right += more_right
    return lax.dot_general(
        jnp.concatenate(left, axis=1),
        jnp.concatenate(right, axis=1),
        (((1,), (1,)), ((), ())),
        preferred_element_type=F32,
    )


def kernel(
    capacity,
    innov_hbm, error_hbm, offset_hbm, cell_hbm, owner_hbm, count_hbm, land_hbm, inertia_hbm, depth_hbm,
    x_ref, r_ref,
    innov_ref, error_ref, offset_ref, cell_ref, owner_ref, count_ref, land_ref, depth_ref, ground_ref,
    sent_ref, inbox_ref, acc_ref, perm_ref,
    tile_ref, pack_ref, strip_ref, pair_ref, edge_ref, side_ref,
    mid_ref, cwest_ref, ceast_ref,
    ocean_ref, diag_ref, cn_ref, cs_ref, cw_ref, ce_ref, q_ref,
    part_ref, slot_ref, gram_ref,
    in_sem, send_sem, recv_sem, halo_send, halo_recv, swap_send, swap_recv, sum_send, sum_recv,
):
    n_lat, n_lon, n_obs = (lax.axis_size(name) for name in AXES)
    lat, lon, core = (lax.axis_index(name) for name in AXES)
    tiles = n_lat * n_lon
    total = tiles * n_obs
    me = (lat * n_lon + lon) * n_obs + core
    rows, cols = x_ref.shape
    tall = rows + 2 * ROW_PAD
    keep = rows + ROW_PAD
    tile_rows = rows * n_obs
    blocks, width = innov_ref.shape
    cap_pad = sent_ref.shape[1]
    fine = fine_size()
    coarse = acc_ref.shape[1]
    group_cols = cols // FINE_COL

    loads = [
        pltpu.make_async_copy(source, target, in_sem.at[number])
        for number, (source, target) in enumerate(
            (
                (count_hbm, count_ref),
                (owner_hbm, owner_ref),
                (innov_hbm, innov_ref),
                (error_hbm, error_ref),
                (offset_hbm, offset_ref),
                (cell_hbm, cell_ref),
                (land_hbm, land_ref),
                (depth_hbm, depth_ref),
                (inertia_hbm, ground_ref.at[1]),
            )
        )
    ]
    for load in loads:
        load.start()

    barrier = pltpu.get_barrier_semaphore()

    def hop_of(ring_step):
        odd = ring_step % 2
        hop = odd * ((ring_step + 1) // 2) + (1 - odd) * (n_lat - ring_step // 2)
        return hop % n_lat

    def everyone(act):
        def line_of(k, carry):
            to_lat = lax.rem(lat + hop_of(n_lat - k), n_lat)
            for shift in range(n_lon):
                to_lon = lax.rem(lon + shift, n_lon)
                for peer in range(n_obs):
                    act((to_lat, to_lon, peer))
            return carry

        lax.fori_loop(1, n_lat, line_of, 0)
        for shift in range(1, n_lon):
            to_lon = lax.rem(lon + shift, n_lon)
            for peer in range(n_obs):
                act((lat, to_lon, peer))
        act((lat, lon, 1 - core))

    everyone(lambda device: pl.semaphore_signal(barrier, inc=1, device_id=device, device_id_type=MESH))

    for load in loads[:2]:
        load.wait()
    count = count_ref[0]
    owner_row = jnp.broadcast_to(owner_ref[...].astype(F32), (blocks, blocks))
    owner_col = owner_row.T
    earlier = (iota((blocks, blocks), 0) < iota((blocks, blocks), 1)) & (
        iota((blocks, blocks), 0) < count
    )
    same = jnp.where((owner_row == owner_col) & earlier, 1.0, 0.0)
    rank = jnp.sum(same, axis=0, keepdims=True)
    slot_of = owner_row[:1] * cap_pad + rank
    slot_of = jnp.where(iota((1, blocks), 1) < count, slot_of, -1.0)
    slots = tiles * cap_pad
    chosen = iota((slots, blocks), 0).astype(F32) == slot_of
    chosen = jnp.where(chosen, 1.0, 0.0).astype(BF16)
    for load in loads[2:6]:
        load.wait()
    error = error_ref[...]
    data = jnp.concatenate(
        [
            innov_ref[...] / (error * error),
            offset_ref[0],
            offset_ref[1],
            cell_ref[...].astype(F32),
        ],
        axis=1,
    )
    high = data.astype(BF16)
    rest = data - high.astype(F32)
    middle = rest.astype(BF16)
    low = (rest - middle.astype(F32)).astype(BF16)
    sent_ref[...] = jnp.dot(
        jnp.concatenate([chosen] * 3, axis=1),
        jnp.concatenate([high, middle, low], axis=0),
        preferred_element_type=F32,
    ).reshape(sent_ref.shape)
    for load in loads[6:]:
        load.wait()
    ground_ref[0] = land_ref[...].astype(F32) * depth_ref[...]
    def block_copy(k):
        hop, shift = hop_of(k // n_lon), k % n_lon
        to_lat, to_lon, bit = (lat + hop) % n_lat, 0, 1
        while bit < n_lon:
            to_lon = to_lon + bit * ((lon // bit + shift // bit) % 2)
            bit = 2 * bit
        moved_over = jnp.where(k == 2, 1 - core, 0)
        slot = k + moved_over * (tiles - 2)
        return pltpu.make_async_remote_copy(
            src_ref=sent_ref.at[to_lat * n_lon + to_lon],
            dst_ref=inbox_ref.at[slot],
            send_sem=send_sem.at[k],
            recv_sem=recv_sem.at[slot],
            device_id=(to_lat, to_lon, core + moved_over),
            device_id_type=MESH,
        )

    def received(k):
        pltpu.make_async_remote_copy(
            src_ref=inbox_ref.at[k],
            dst_ref=inbox_ref.at[k],
            send_sem=send_sem.at[0],
            recv_sem=recv_sem.at[k],
            device_id=(lat, lon, 1 - core),
            device_id_type=MESH,
        ).wait_recv()
        return inbox_ref[k]

    def send(k, carry):
        block_copy(k).start()
        return carry

    def halo_copy(index, source, target, device):
        return pltpu.make_async_remote_copy(
            src_ref=source,
            dst_ref=target,
            send_sem=halo_send.at[index],
            recv_sem=halo_recv.at[index],
            device_id=device,
            device_id_type=MESH,
        )

    line = lat * n_obs + core
    last_line = n_lat * n_obs - 1
    above = jnp.maximum(line - 1, 0)
    below = jnp.minimum(line + 1, last_line)
    above = (above // n_obs, above % n_obs)
    below = (below // n_obs, below % n_obs)
    west = lax.rem(lon + n_lon - 1, n_lon)
    east = lax.rem(lon + 1, n_lon)
    first_rows, last_rows = pl.ds(0, ROW_PAD), pl.ds(rows - ROW_PAD, ROW_PAD)
    first_cols, last_cols = pl.ds(0, COL_PAD), pl.ds(cols - COL_PAD, COL_PAD)
    row_before, row_after = pl.ds(0, ROW_PAD), pl.ds(keep, ROW_PAD)
    inside = pl.ds(ROW_PAD, rows)

    def across_lon(number, source_rows, target_rows, to_lat, to_core):
        return [
            halo_copy(
                number,
                ground_ref.at[:, source_rows, last_cols],
                cwest_ref.at[:, target_rows],
                (to_lat, east, to_core),
            ),
            halo_copy(
                number + 1,
                ground_ref.at[:, source_rows, first_cols],
                ceast_ref.at[:, target_rows],
                (to_lat, west, to_core),
            ),
        ]

    level_halo = across_lon(0, pl.ds(0, rows), inside, lat, core)

    def halo_above():
        to_lat, to_core = above
        return [
            halo_copy(2, ground_ref.at[:, first_rows], mid_ref.at[:, row_after], (to_lat, lon, to_core))
        ] + across_lon(3, first_rows, row_after, to_lat, to_core)

    def halo_below():
        to_lat, to_core = below
        return [
            halo_copy(5, ground_ref.at[:, last_rows], mid_ref.at[:, row_before], (to_lat, lon, to_core))
        ] + across_lon(6, last_rows, row_before, to_lat, to_core)

    def post_sum(turn, parts):
        stack = jnp.concatenate(
            parts + [jnp.zeros((COL_PAD - 8 * len(parts), COL_PAD), F32)], axis=0
        )
        values = jnp.sum(stack.T, axis=0, keepdims=True)
        slot_ref[turn, pl.ds(me, 1)] = values[None]
        part_ref[turn] = values

        everyone(
            lambda device: pltpu.make_async_remote_copy(
                src_ref=part_ref.at[turn],
                dst_ref=slot_ref.at[turn, me],
                send_sem=sum_send.at[turn],
                recv_sem=sum_recv.at[turn],
                device_id=device,
                device_id_type=MESH,
            ).start()
        )

    def take_sum(turn, number):
        block = slot_ref.at[turn, pl.ds(0, total - 1)]
        pltpu.make_async_copy(block, block, sum_recv.at[turn]).wait()
        pltpu.make_async_copy(block, block, sum_send.at[turn]).wait()
        values = jnp.sum(slot_ref[turn], axis=0)
        gram_ref[...] = jnp.broadcast_to(values, (COL_PAD, COL_PAD)).T
        return [
            jnp.sum(gram_ref[8 * k : 8 * k + 8], axis=0, keepdims=True) for k in range(number)
        ]

    def fold(value):
        out = value[:8]
        for start in range(8, rows, 8):
            out = out + value[start : start + 8]
        lanes = out[:, :COL_PAD]
        for start in range(COL_PAD, cols, COL_PAD):
            lanes = lanes + out[:, start : start + COL_PAD]
        return lanes

    def spread(*blocks):
        return spread_blocks(capacity, width, cols, coarse, blocks)

    pl.semaphore_wait(barrier, total - 1)
    lax.fori_loop(1, tiles, send, 0)
    for item in level_halo:
        item.start()

    @pl.when(line > 0)
    def _():
        for item in halo_above():
            item.start()

    @pl.when(line < last_line)
    def _():
        for item in halo_below():
            item.start()

    acc_ref[...] = spread(sent_ref[lat * n_lon + lon])

    def fill(part, carry):
        shape = (group_cols, cols)
        target = iota(shape, 0) * FINE_COL + part
        start = pl.multiple_of(part * group_cols, group_cols)
        perm_ref[pl.ds(start, group_cols)] = jnp.where(target == iota(shape, 1), 1.0, 0.0).astype(BF16)
        return carry

    lax.fori_loop(0, FINE_COL, fill, 0)

    conduct = ground_ref[0]
    kept = jnp.where(conduct > 0.0, 1.0, 0.0)
    row_face = conduct * moved(conduct, 0, False)
    col_face = conduct * moved(conduct, 1, False)
    faces = row_face + moved(row_face, 0, True) + col_face + moved(col_face, 1, True)
    row_face = jnp.sqrt(row_face)
    col_face = jnp.sqrt(col_face)
    center = ground_ref[1] + row_face + moved(row_face, 0, True) + col_face + moved(col_face, 1, True)
    center = center * kept
    post_sum(0, [fold(kept), fold(center), fold(center * center), fold(faces)])

    def gather(*slots):
        acc_ref[...] = acc_ref[...] + spread(*[received(k) for k in slots])

    @pl.when(core == 0)
    def _():
        gather(1)

    @pl.when(core == 1)
    def _():
        gather(1, 2)

    def two(k, carry):
        gather(2 * k + 1, 2 * k + 2)
        return carry

    lax.fori_loop(1, tiles // 2 - 1, two, 0)

    @pl.when(core == 0)
    def _():
        gather(tiles - 1)

    @pl.when(core == 1)
    def _():
        gather(tiles - 1, tiles)

    acc_ref[:fine] = acc_ref[:fine] + acc_ref[fine:]
    step = FINE_ROW + 1
    top_row = iota((8, group_cols), 0) == 0
    blank = jnp.zeros((FINE_ROW - 8, group_cols), F32)
    planes = []
    for part in range(FINE_COL + 1):
        pieces, spill = [], None
        for index in range(tile_rows // FINE_ROW):
            lanes = slice(index * group_cols, (index + 1) * group_cols)
            piece = acc_ref[part * step : part * step + FINE_ROW, lanes]
            if spill is not None:
                piece = piece + jnp.concatenate([spill, blank], axis=0)
            pieces.append(piece)
            last = acc_ref[part * step + FINE_ROW : part * step + step, lanes]
            spill = jnp.where(top_row, last, 0.0)
        planes.append(jnp.concatenate(pieces + [spill], axis=0))
    over = pltpu.roll(planes[FINE_COL], 1, 1)
    lane = iota(over.shape, 1)
    planes[0] = planes[0] + jnp.where(lane > 0, over, 0.0)
    beyond = jnp.where(lane == 0, over, 0.0)
    mixed = jnp.concatenate(planes[:FINE_COL], axis=1)
    high = mixed.astype(BF16).astype(F32)
    mixed = jnp.concatenate([high, mixed - high], axis=0).astype(BF16)
    natural = jnp.dot(mixed, perm_ref[...], preferred_element_type=F32)
    tile_tall = tile_rows + ROW_PAD
    natural = natural[:tile_tall] + natural[tile_tall:]
    tile_ref[:, :cols] = natural
    tile_ref[:, cols:] = beyond
    top = iota((ROW_PAD, cols + COL_PAD), 0) == 0
    pack_ref[...] = jnp.where(
        top, tile_ref[tile_rows:], tile_ref[tile_rows - ROW_PAD : tile_rows]
    )
    sides = jnp.where(lane < COL_PAD // 2, natural[:, :COL_PAD], natural[:, cols - COL_PAD :])
    sides = jnp.where(lane == COL_PAD - 8, pltpu.roll(beyond, COL_PAD - 8, 1), sides)
    sides = jnp.concatenate([sides, jnp.zeros((COL_PAD - tile_tall, COL_PAD), F32)], axis=0)
    strip_ref[...] = sides.T

    split = rows - ROW_PAD
    mine = pl.multiple_of(core * split, 8)
    theirs = pl.multiple_of((1 - core) * split, 8)
    north = lat > 0
    south = lat < n_lat - 1
    from_west = strip_ref.at[pl.ds(0, 8)]
    from_east = strip_ref.at[pl.ds(COL_PAD - 8, 8)]

    def swap_copy(out, into, source, target, device):
        return pltpu.make_async_remote_copy(
            src_ref=source,
            dst_ref=target,
            send_sem=swap_send.at[out],
            recv_sem=swap_recv.at[into],
            device_id=device,
            device_id_type=MESH,
        )

    up_lat, down_lat = jnp.maximum(lat - 1, 0), jnp.minimum(lat + 1, n_lat - 1)

    def northern():
        return [
            swap_copy(1, 1 + core, tile_ref.at[pl.ds(0, 8)], edge_ref.at[core], (up_lat, lon, 1)),
            swap_copy(2, 3 + core, from_west, side_ref.at[2 + core], (up_lat, west, 1)),
            swap_copy(3, 5 + core, from_east, side_ref.at[6 + core], (up_lat, east, 1)),
        ]

    def southern():
        return [
            swap_copy(4, 1 + core, pack_ref, edge_ref.at[core], (down_lat, lon, 0)),
            swap_copy(5, 3 + core, from_west, side_ref.at[2 + core], (down_lat, west, 0)),
            swap_copy(6, 5 + core, from_east, side_ref.at[6 + core], (down_lat, east, 0)),
        ]

    level = [
        swap_copy(7 + peer, 7 + core, from_west, side_ref.at[core], (lat, west, peer))
        for peer in range(2)
    ] + [
        swap_copy(9 + peer, 9 + core, from_east, side_ref.at[4 + core], (lat, east, peer))
        for peer in range(2)
    ]
    swap = swap_copy(0, 0, tile_ref.at[pl.ds(theirs, tall)], pair_ref, (lat, lon, 1 - core))

    @pl.when(north)
    def _():
        for item in northern():
            item.start()

    @pl.when(south)
    def _():
        for item in southern():
            item.start()

    for item in level:
        item.start()
    swap.start()

    mid_ref[:, inside] = ground_ref[...]

    @pl.when(line > 0)
    def _():
        for item in halo_below():
            item.wait_recv()

    @pl.when(line < last_line)
    def _():
        for item in halo_above():
            item.wait_recv()

    @pl.when(line == 0)
    def _():
        for ref in (mid_ref, cwest_ref, ceast_ref):
            ref[:, row_before] = jnp.zeros_like(ref[:, row_before])

    @pl.when(line == last_line)
    def _():
        for ref in (mid_ref, cwest_ref, ceast_ref):
            ref[:, row_after] = jnp.zeros_like(ref[:, row_after])

    for item in level_halo:
        item.wait_recv()
    near = iota((tall, COL_PAD), 1) < COL_PAD // 2

    def widened(index):
        pad = jnp.where(near, ceast_ref[index], cwest_ref[index])
        return jnp.concatenate([mid_ref[index], pad], axis=1)

    conduct = widened(0)
    cn = jnp.sqrt(conduct * moved(conduct, 0, False))
    cs = moved(cn, 0, True)
    cw = jnp.sqrt(conduct * moved(conduct, 1, False))
    ce = moved(cw, 1, True)
    cn_ref[...] = cn
    cs_ref[...] = cs
    cw_ref[...] = cw
    ce_ref[...] = ce
    ocean_ref[...] = jnp.where(conduct > 0.0, 1.0, 0.0)
    diag_ref[...] = widened(1) + cn + cs + cw + ce

    ocean_count, diag_sum, diag_square, face_square = take_sum(0, 4)
    ocean_count = jnp.maximum(ocean_count, 1.0)
    mean = diag_sum / ocean_count
    spread_out = jnp.maximum((diag_square + face_square) / ocean_count - mean * mean, 0.0)
    mean = 1.2 * mean

    def across(value, size):
        return jnp.concatenate([value] * (size // COL_PAD), axis=1)

    diag_ref[...] = diag_ref[...] - across(mean, cols + COL_PAD)

    def finish(k, carry):
        block_copy(k).wait_send()
        return carry

    lax.fori_loop(1, tiles, finish, 0)
    for item in level_halo:
        item.wait_send()

    @pl.when(line > 0)
    def _():
        for item in halo_above():
            item.wait_send()

    @pl.when(line < last_line)
    def _():
        for item in halo_below():
            item.wait_send()

    linked = jnp.where(core == 0, lat, n_lat - 1 - lat) > 0

    def arrived(number, target):
        return swap_copy(0, number, target, target, (lat, lon, 1 - core))

    @pl.when(linked)
    def _():
        for sender in range(2):
            arrived(1 + sender, edge_ref.at[sender]).wait_recv()
            arrived(3 + sender, side_ref.at[2 + sender]).wait_recv()
            arrived(5 + sender, side_ref.at[6 + sender]).wait_recv()

    @pl.when(jnp.logical_not(linked))
    def _():
        edge_ref[...] = jnp.zeros_like(edge_ref)
        side_ref[2:4] = jnp.zeros((2, 8, COL_PAD), F32)
        side_ref[6:8] = jnp.zeros((2, 8, COL_PAD), F32)

    for sender in range(2):
        arrived(7 + sender, side_ref.at[sender]).wait_recv()
        arrived(9 + sender, side_ref.at[4 + sender]).wait_recv()

    def aligned(straight, corner):
        first = core == 0
        straight = jnp.where(
            first, pltpu.roll(straight, ROW_PAD, 1), pltpu.roll(straight, COL_PAD - split, 1)
        )
        corner = jnp.where(
            first,
            pltpu.roll(corner, COL_PAD - (tile_rows - ROW_PAD), 1),
            pltpu.roll(corner, keep, 1),
        )
        return straight + corner

    right_side = aligned(side_ref[0] + side_ref[1], side_ref[2] + side_ref[3])
    left_side = aligned(side_ref[4] + side_ref[5], side_ref[6] + side_ref[7])
    hole = jnp.zeros((COL_PAD - 16, COL_PAD), F32)
    beside = jnp.concatenate([right_side, hole, left_side], axis=0).T[:tall]
    entering = jnp.where(iota(beside.shape, 1) == 0, pltpu.roll(beside, 8, 1), 0.0)
    edge = edge_ref[0] + edge_ref[1]
    swap.wait_recv()

    @pl.when(core == 0)
    def _():
        q_ref[0, :ROW_PAD] = jnp.where(top, 0.0, edge)
        q_ref[0, ROW_PAD : 2 * ROW_PAD] = (
            tile_ref[:ROW_PAD] + pair_ref[:ROW_PAD] + jnp.where(top, edge, 0.0)
        )
        q_ref[0, 2 * ROW_PAD :] = tile_ref[ROW_PAD:keep] + pair_ref[ROW_PAD:keep]

    @pl.when(core == 1)
    def _():
        q_ref[0, :keep] = tile_ref[pl.ds(split, keep)] + pair_ref[:keep]
        q_ref[0, keep:] = tile_ref[pl.ds(split + keep, ROW_PAD)] + pair_ref[keep:] + edge

    q_ref[0, :, :COL_PAD] = q_ref[0, :, :COL_PAD] + entering
    q_ref[0, :, cols:] = q_ref[0, :, cols:] + beside
    q_ref[0] = q_ref[0] * ocean_ref[...]

    spread_wide = across(spread_out, cols + COL_PAD)
    for k in range(ITERS):
        field = q_ref[k]
        value = (
            diag_ref[...] * field
            - cn_ref[...] * moved(field, 0, False)
            - cs_ref[...] * moved(field, 0, True)
            - cw_ref[...] * moved(field, 1, False)
            - ce_ref[...] * moved(field, 1, True)
        )
        if k:
            value = value - spread_wide * q_ref[k - 1]
        q_ref[k + 1] = value

    fields = [q_ref[k, ROW_PAD:keep, :cols] for k in range(ITERS + 1)]
    pairs = [(k, k + d) for k in range(ITERS) for d in range(2)]
    post_sum(1, [fold(fields[i] * fields[j]) for i, j in pairs])
    swap.wait_send()
    for item in level:
        item.wait_send()

    @pl.when(north)
    def _():
        for item in northern():
            item.wait_send()

    @pl.when(south)
    def _():
        for item in southern():
            item.wait_send()

    sums = take_sum(1, len(pairs))
    gram = {}
    for (i, j), value in zip(pairs, sums):
        gram[i, j] = gram[j, i] = value
    for gap in range(1, ITERS):
        for i in range(ITERS - gap):
            j = i + gap
            value = gram[i + 1, j]
            if i:
                value = value + spread_out * (gram[i - 1, j] - gram[i, j - 1])
            else:
                value = value - spread_out * gram[i, j - 1]
            gram[i, j + 1] = gram[j + 1, i] = value

    def plus(one, two):
        if one is None or two is None:
            return two if one is None else one
        return one + two

    def times(weight, part):
        return None if part is None else weight * part

    def quad(first, second):
        out = None
        for i, one in enumerate(first):
            line = None
            for j, two in enumerate(second):
                if one is not None and two is not None:
                    line = plus(line, two * gram[i, j])
            out = plus(out, times(one, line) if one is not None else None)
        return out

    def apply(weights):
        out = [None] * (ITERS + 1)
        for k, weight in enumerate(weights[:ITERS]):
            if weight is not None:
                out[k + 1] = plus(out[k + 1], weight)
                out[k] = plus(out[k], mean * weight)
                if k:
                    out[k - 1] = plus(out[k - 1], spread_out * weight)
        return out

    unit = jnp.ones((1, COL_PAD), F32)
    direct = [unit] + [None] * ITERS
    resid = [unit] + [None] * ITERS
    gained = [None] * (ITERS + 1)
    norm = gram[0, 0]
    for done in range(1, ITERS + 1):
        applied = apply(direct)
        step_size = norm / quad(direct, applied)
        gained = [plus(one, times(step_size, two)) for one, two in zip(gained, direct)]
        resid = [plus(one, times(-step_size, two)) for one, two in zip(resid, applied)]
        if done < ITERS:
            norm_next = quad(resid, resid)
            ratio = norm_next / norm
            direct = [plus(one, times(ratio, two)) for one, two in zip(resid, direct)]
            norm = norm_next

    def mix(weights):
        out = None
        for k, weight in enumerate(weights):
            if weight is not None:
                out = plus(out, across(weight, cols) * q_ref[k, ROW_PAD:keep, :cols])
        return out

    x_ref[...] = mix(gained)
    r_ref[...] = mix(resid)


def write(x_ref, r_ref, x_hbm, r_hbm, sem):
    copies = [
        pltpu.make_async_copy(x_ref, x_hbm, sem.at[0]),
        pltpu.make_async_copy(r_ref, r_hbm, sem.at[1]),
    ]
    for copy in copies:
        copy.start()
    for copy in copies:
        copy.wait()


def body(
    innovation, obs_error, obs_offset, obs_cell, obs_owner, block_count,
    land_mask, inertia, sea_depth,
):
    block_total = obs_owner.shape[1]
    width = innovation.shape[1]
    n_lat, n_lon, n_obs = (lax.axis_size(name) for name in AXES)
    tiles = n_lat * n_lon
    capacity = max(3, 2 * ((block_total + tiles - 1) // tiles))
    cap_pad = -(-capacity // 8) * 8
    rows, cols = land_mask.shape
    total = tiles * n_obs
    coarse = (rows * n_obs // FINE_ROW) * (cols // FINE_COL)
    tall, broad = rows + 2 * ROW_PAD, cols + COL_PAD
    tile_tall = rows * n_obs + ROW_PAD
    vmem = lambda *shape: pltpu.VMEM(shape, F32)
    whole = pl.BlockSpec(memory_space=pltpu.VMEM)
    far = pl.BlockSpec(memory_space=pltpu.HBM)
    dma = pltpu.SemaphoreType.DMA
    fields = pl.pallas_call(
        functools.partial(kernel, capacity),
        out_shape=[pltpu.VMEM((rows, cols), F32)] * 2,
        in_specs=[far] * 9,
        out_specs=[whole] * 2,
        scratch_shapes=[
            vmem(*innovation.shape),
            vmem(*obs_error.shape),
            vmem(*obs_offset.shape),
            pltpu.VMEM(obs_cell.shape, jnp.int32),
            pltpu.VMEM(obs_owner.shape, jnp.int32),
            pltpu.SMEM(block_count.shape, jnp.int32),
            pltpu.VMEM((rows, cols), jnp.int32),
            vmem(rows, cols),
            vmem(2, rows, cols),
            vmem(tiles, cap_pad, 4 * width),
            vmem(tiles + 1, cap_pad, 4 * width),
            vmem(2 * fine_size(), coarse),
            pltpu.VMEM((cols, cols), BF16),
            vmem(tile_tall, broad),
            vmem(ROW_PAD, broad),
            vmem(COL_PAD, COL_PAD),
            vmem(tall, broad),
            vmem(2, ROW_PAD, broad),
            vmem(8, 8, COL_PAD),
            vmem(2, tall, cols),
            vmem(2, tall, COL_PAD),
            vmem(2, tall, COL_PAD),
        ]
        + [vmem(tall, broad)] * 6
        + [
            vmem(ITERS + 1, tall, broad),
            vmem(2, 1, COL_PAD),
            vmem(2, total, 1, COL_PAD),
            vmem(COL_PAD, COL_PAD),
            dma((9,)),
            dma((tiles,)),
            dma((tiles + 1,)),
            dma((8,)),
            dma((8,)),
            dma((11,)),
            dma((11,)),
            dma((2,)),
            dma((2,)),
        ],
        compiler_params=pltpu.CompilerParams(collective_id=0, has_side_effects=True),
        name="adjoint",
    )(
        innovation, obs_error, obs_offset, obs_cell, obs_owner, block_count,
        land_mask, inertia, sea_depth,
    )
    return pl.pallas_call(
        write,
        out_shape=[jax.ShapeDtypeStruct((rows, cols), F32)] * 2,
        in_specs=[whole] * 2,
        out_specs=[far] * 2,
        scratch_shapes=[dma((2,))],
        name="write",
    )(*[pltpu.with_memory_space_constraint(field, pltpu.VMEM) for field in fields])


def solution(mesh):
    spread = P(AXES, None)
    grid = P(("lat", "obs"), "lon")
    in_specs = (spread, spread, P(None, AXES, None), spread, spread, P(AXES), grid, grid, grid)
    return jax.shard_map(
        body, mesh=mesh, in_specs=in_specs, out_specs=(grid, grid), check_vma=False
    )
```

```python
import functools

import jax
import jax.numpy as jnp
from jax import lax
from jax.experimental import pallas as pl
from jax.experimental.pallas import tpu as pltpu
from jax.sharding import PartitionSpec as P

ITERS = 5
ROW_PAD = 8
COL_PAD = 128
FINE_ROW = 16
FINE_COL = 8
MESH = pl.DeviceIdType.MESH
AXES = ("lat", "lon", "obs")
F32 = jnp.float32
BF16 = jnp.bfloat16


def iota(shape, axis):
    return lax.broadcasted_iota(jnp.int32, shape, axis)


def moved(value, axis, back):
    size = value.shape[axis]
    return pltpu.roll(value, size - 1 if back else 1, axis)


def fine_size():
    return -(-(FINE_ROW + 1) * (FINE_COL + 1) // 16) * 16


def operands(capacity, width, cols, coarse, block):
    fine = fine_size()
    amount = block[:, :width]
    north = block[:, width : 2 * width]
    east = block[:, 2 * width : 3 * width]
    cell = block[:, 3 * width :]
    row = jnp.floor(cell * (1.0 / cols))
    col = cell - row * cols
    row_group = jnp.floor(row * (1.0 / FINE_ROW))
    col_group = jnp.floor(col * (1.0 / FINE_COL))
    step = FINE_ROW + 1
    first = (col - col_group * FINE_COL) * step + (row - row_group * FINE_ROW)
    group = row_group * (cols // FINE_COL) + col_group - coarse // 2
    upper = amount * (1.0 - north)
    lower = amount * north
    corners = []
    for shift, part in (
        (0, upper * (1.0 - east)),
        (1, lower * (1.0 - east)),
        (step, upper * east),
        (step + 1, lower * east),
    ):
        high = part.astype(BF16).astype(F32)
        corners.append((first + shift, high, part - high))

    def wide(values, slot, count):
        tile = jnp.broadcast_to(values[slot : slot + 1], (16, width)).astype(BF16)
        return jnp.concatenate([tile] * (count // 16), axis=0)

    fine_axis = iota((fine, width), 0).astype(F32).astype(BF16)
    coarse_axis = (iota((coarse, width), 0) - coarse // 2).astype(F32).astype(BF16)
    zero = jnp.zeros((), BF16)
    one = jnp.ones((), BF16)
    left, right = [], []
    for slot in range(capacity):
        high = low = zero
        for place, top, rest in corners:
            hit = fine_axis == wide(place, slot, fine)
            high = jnp.where(hit, wide(top, slot, fine), high)
            low = jnp.where(hit, wide(rest, slot, fine), low)
        left.append(jnp.concatenate([high, low], axis=0))
        right.append(jnp.where(coarse_axis == wide(group, slot, coarse), one, zero))
    return left, right


def spread_blocks(capacity, width, cols, coarse, blocks):
    left, right = [], []
    for block in blocks:
        more_left, more_right = operands(capacity, width, cols, coarse, block)
        left += more_left
        right += more_right
    return lax.dot_general(
        jnp.concatenate(left, axis=1),
        jnp.concatenate(right, axis=1),
        (((1,), (1,)), ((), ())),
        preferred_element_type=F32,
    )


def kernel(
    capacity,
    innov_hbm, error_hbm, offset_hbm, cell_hbm, owner_hbm, count_hbm, land_hbm, inertia_hbm, depth_hbm,
    x_ref, r_ref,
    innov_ref, error_ref, offset_ref, cell_ref, owner_ref, count_ref, land_ref, depth_ref, ground_ref,
    sent_ref, inbox_ref, acc_ref, perm_ref,
    tile_ref, pack_ref, strip_ref, pair_ref, edge_ref, side_ref,
    mid_ref, cwest_ref, ceast_ref,
    ocean_ref, diag_ref, cn_ref, cs_ref, cw_ref, ce_ref, q_ref,
    part_ref, slot_ref, gram_ref,
    in_sem, send_sem, recv_sem, halo_send, halo_recv, swap_send, swap_recv, sum_send, sum_recv,
):
    n_lat, n_lon, n_obs = (lax.axis_size(name) for name in AXES)
    lat, lon, core = (lax.axis_index(name) for name in AXES)
    tiles = n_lat * n_lon
    total = tiles * n_obs
    me = (lat * n_lon + lon) * n_obs + core
    rows, cols = x_ref.shape
    tall = rows + 2 * ROW_PAD
    keep = rows + ROW_PAD
    tile_rows = rows * n_obs
    blocks, width = innov_ref.shape
    cap_pad = sent_ref.shape[1]
    fine = fine_size()
    coarse = acc_ref.shape[1]
    group_cols = cols // FINE_COL

    loads = [
        pltpu.make_async_copy(source, target, in_sem.at[number])
        for number, (source, target) in enumerate(
            (
                (count_hbm, count_ref),
                (owner_hbm, owner_ref),
                (innov_hbm, innov_ref),
                (error_hbm, error_ref),
                (offset_hbm, offset_ref),
                (cell_hbm, cell_ref),
                (land_hbm, land_ref),
                (depth_hbm, depth_ref),
                (inertia_hbm, ground_ref.at[1]),
            )
        )
    ]
    for load in loads:
        load.start()

    barrier = pltpu.get_barrier_semaphore()

    def hop_of(ring_step):
        odd = ring_step % 2
        hop = odd * ((ring_step + 1) // 2) + (1 - odd) * (n_lat - ring_step // 2)
        return hop % n_lat

    def everyone(act):
        def line_of(k, carry):
            to_lat = lax.rem(lat + hop_of(n_lat - k), n_lat)
            for shift in range(n_lon):
                to_lon = lax.rem(lon + shift, n_lon)
                for peer in range(n_obs):
                    act((to_lat, to_lon, peer))
            return carry

        lax.fori_loop(1, n_lat, line_of, 0)
        for shift in range(1, n_lon):
            to_lon = lax.rem(lon + shift, n_lon)
            for peer in range(n_obs):
                act((lat, to_lon, peer))
        act((lat, lon, 1 - core))

    everyone(lambda device: pl.semaphore_signal(barrier, inc=1, device_id=device, device_id_type=MESH))

    for load in loads[:2]:
        load.wait()
    count = count_ref[0]
    owner_row = jnp.broadcast_to(owner_ref[...].astype(F32), (blocks, blocks))
    owner_col = owner_row.T
    earlier = (iota((blocks, blocks), 0) < iota((blocks, blocks), 1)) & (
        iota((blocks, blocks), 0) < count
    )
    same = jnp.where((owner_row == owner_col) & earlier, 1.0, 0.0)
    rank = jnp.sum(same, axis=0, keepdims=True)
    slot_of = owner_row[:1] * cap_pad + rank
    slot_of = jnp.where(iota((1, blocks), 1) < count, slot_of, -1.0)
    slots = tiles * cap_pad
    chosen = iota((slots, blocks), 0).astype(F32) == slot_of
    chosen = jnp.where(chosen, 1.0, 0.0).astype(BF16)
    for load in loads[2:6]:
        load.wait()
    error = error_ref[...]
    data = jnp.concatenate(
        [
            innov_ref[...] / (error * error),
            offset_ref[0],
            offset_ref[1],
            cell_ref[...].astype(F32),
        ],
        axis=1,
    )
    high = data.astype(BF16)
    rest = data - high.astype(F32)
    middle = rest.astype(BF16)
    low = (rest - middle.astype(F32)).astype(BF16)
    sent_ref[...] = jnp.dot(
        jnp.concatenate([chosen] * 3, axis=1),
        jnp.concatenate([high, middle, low], axis=0),
        preferred_element_type=F32,
    ).reshape(sent_ref.shape)
    for load in loads[6:]:
        load.wait()
    ground_ref[0] = land_ref[...].astype(F32) * depth_ref[...]
    def block_copy(k):
        hop, shift = hop_of(k // n_lon), k % n_lon
        to_lat, to_lon, bit = (lat + hop) % n_lat, 0, 1
        while bit < n_lon:
            to_lon = to_lon + bit * ((lon // bit + shift // bit) % 2)
            bit = 2 * bit
        moved_over = jnp.where(k == 2, 1 - core, 0)
        slot = k + moved_over * (tiles - 2)
        return pltpu.make_async_remote_copy(
            src_ref=sent_ref.at[to_lat * n_lon + to_lon],
            dst_ref=inbox_ref.at[slot],
            send_sem=send_sem.at[k],
            recv_sem=recv_sem.at[slot],
            device_id=(to_lat, to_lon, core + moved_over),
            device_id_type=MESH,
        )

    def received(turn):
        k = jnp.where(turn == n_lon + 2, 1, turn)
        k = jnp.where((turn > n_lon + 2) & (turn < 2 * n_lon), turn - n_lon, k)
        k = jnp.where((turn > 2) & (turn < n_lon + 2), turn + n_lon - 2, k)
        k = jnp.where(turn == 1, n_lon, k)
        k = jnp.where(early, k, turn)
        pltpu.make_async_remote_copy(
            src_ref=inbox_ref.at[k],
            dst_ref=inbox_ref.at[k],
            send_sem=send_sem.at[0],
            recv_sem=recv_sem.at[k],
            device_id=(lat, lon, 1 - core),
            device_id_type=MESH,
        ).wait_recv()
        return inbox_ref[k]

    def send(k, carry):
        block_copy(k).start()
        return carry

    def halo_copy(index, source, target, device):
        return pltpu.make_async_remote_copy(
            src_ref=source,
            dst_ref=target,
            send_sem=halo_send.at[index],
            recv_sem=halo_recv.at[index],
            device_id=device,
            device_id_type=MESH,
        )

    line = lat * n_obs + core
    last_line = n_lat * n_obs - 1
    above = jnp.maximum(line - 1, 0)
    below = jnp.minimum(line + 1, last_line)
    above = (above // n_obs, above % n_obs)
    below = (below // n_obs, below % n_obs)
    west = lax.rem(lon + n_lon - 1, n_lon)
    east = lax.rem(lon + 1, n_lon)
    first_rows, last_rows = pl.ds(0, ROW_PAD), pl.ds(rows - ROW_PAD, ROW_PAD)
    first_cols, last_cols = pl.ds(0, COL_PAD), pl.ds(cols - COL_PAD, COL_PAD)
    row_before, row_after = pl.ds(0, ROW_PAD), pl.ds(keep, ROW_PAD)
    inside = pl.ds(ROW_PAD, rows)

    def across_lon(number, source_rows, target_rows, to_lat, to_core):
        return [
            halo_copy(
                number,
                ground_ref.at[:, source_rows, last_cols],
                cwest_ref.at[:, target_rows],
                (to_lat, east, to_core),
            ),
            halo_copy(
                number + 1,
                ground_ref.at[:, source_rows, first_cols],
                ceast_ref.at[:, target_rows],
                (to_lat, west, to_core),
            ),
        ]

    level_halo = across_lon(0, pl.ds(0, rows), inside, lat, core)

    def halo_above():
        to_lat, to_core = above
        return [
            halo_copy(2, ground_ref.at[:, first_rows], mid_ref.at[:, row_after], (to_lat, lon, to_core))
        ] + across_lon(3, first_rows, row_after, to_lat, to_core)

    def halo_below():
        to_lat, to_core = below
        return [
            halo_copy(5, ground_ref.at[:, last_rows], mid_ref.at[:, row_before], (to_lat, lon, to_core))
        ] + across_lon(6, last_rows, row_before, to_lat, to_core)

    def post_sum(turn, parts):
        stack = jnp.concatenate(
            parts + [jnp.zeros((COL_PAD - 8 * len(parts), COL_PAD), F32)], axis=0
        )
        values = jnp.sum(stack.T, axis=0, keepdims=True)
        slot_ref[turn, pl.ds(me, 1)] = values[None]
        part_ref[turn] = values

        everyone(
            lambda device: pltpu.make_async_remote_copy(
                src_ref=part_ref.at[turn],
                dst_ref=slot_ref.at[turn, me],
                send_sem=sum_send.at[turn],
                recv_sem=sum_recv.at[turn],
                device_id=device,
                device_id_type=MESH,
            ).start()
        )

    def take_sum(turn, number):
        block = slot_ref.at[turn, pl.ds(0, total - 1)]
        pltpu.make_async_copy(block, block, sum_recv.at[turn]).wait()
        pltpu.make_async_copy(block, block, sum_send.at[turn]).wait()
        values = jnp.sum(slot_ref[turn], axis=0)
        gram_ref[...] = jnp.broadcast_to(values, (COL_PAD, COL_PAD)).T
        return [
            jnp.sum(gram_ref[8 * k : 8 * k + 8], axis=0, keepdims=True) for k in range(number)
        ]

    def fold(value):
        out = value[:8]
        for start in range(8, rows, 8):
            out = out + value[start : start + 8]
        lanes = out[:, :COL_PAD]
        for start in range(COL_PAD, cols, COL_PAD):
            lanes = lanes + out[:, start : start + COL_PAD]
        return lanes

    def spread(*blocks):
        return spread_blocks(capacity, width, cols, coarse, blocks)

    early = lat < (n_lat + 3) // 4

    @pl.when(early)
    def _():
        acc_ref[...] = spread(sent_ref[lat * n_lon + lon])

    pl.semaphore_wait(barrier, total - 1)
    lax.fori_loop(1, tiles, send, 0)
    for item in level_halo:
        item.start()

    @pl.when(line > 0)
    def _():
        for item in halo_above():
            item.start()

    @pl.when(line < last_line)
    def _():
        for item in halo_below():
            item.start()

    @pl.when(jnp.logical_not(early))
    def _():
        acc_ref[...] = spread(sent_ref[lat * n_lon + lon])

    span = perm_ref.shape[0]
    chunk = span // FINE_COL
    index = iota((span, span), 0)
    target = index % chunk * FINE_COL + index // chunk
    perm_ref[...] = jnp.where(target == iota((span, span), 1), 1.0, 0.0).astype(BF16)

    conduct = ground_ref[0]
    kept = jnp.where(conduct > 0.0, 1.0, 0.0)
    row_face = conduct * moved(conduct, 0, False)
    col_face = conduct * moved(conduct, 1, False)
    faces = row_face + moved(row_face, 0, True) + col_face + moved(col_face, 1, True)
    row_face = jnp.sqrt(row_face)
    col_face = jnp.sqrt(col_face)
    center = ground_ref[1] + row_face + moved(row_face, 0, True) + col_face + moved(col_face, 1, True)
    center = center * kept
    post_sum(0, [fold(kept), fold(center), fold(center * center), fold(faces)])

    def gather(*slots):
        acc_ref[...] = acc_ref[...] + spread(*[received(k) for k in slots])

    @pl.when(core == 0)
    def _():
        gather(1)

    @pl.when(core == 1)
    def _():
        gather(1, 2)

    def two(k, carry):
        gather(2 * k + 1, 2 * k + 2)
        return carry

    lax.fori_loop(1, tiles // 2 - 1, two, 0)

    @pl.when(core == 0)
    def _():
        gather(tiles - 1)

    @pl.when(core == 1)
    def _():
        gather(tiles - 1, tiles)

    acc_ref[:fine] = acc_ref[:fine] + acc_ref[fine:]
    step = FINE_ROW + 1
    top_row = iota((8, group_cols), 0) == 0
    blank = jnp.zeros((FINE_ROW - 8, group_cols), F32)
    planes = []
    for part in range(FINE_COL + 1):
        pieces, spill = [], None
        for index in range(tile_rows // FINE_ROW):
            lanes = slice(index * group_cols, (index + 1) * group_cols)
            piece = acc_ref[part * step : part * step + FINE_ROW, lanes]
            if spill is not None:
                piece = piece + jnp.concatenate([spill, blank], axis=0)
            pieces.append(piece)
            last = acc_ref[part * step + FINE_ROW : part * step + step, lanes]
            spill = jnp.where(top_row, last, 0.0)
        planes.append(jnp.concatenate(pieces + [spill], axis=0))
    over = pltpu.roll(planes[FINE_COL], 1, 1)
    lane = iota(over.shape, 1)
    planes[0] = planes[0] + jnp.where(lane > 0, over, 0.0)
    beyond = jnp.where(lane == 0, over, 0.0)
    fit = group_cols // chunk
    mixed = []
    for run in range(cols // span):
        halves = []
        for half in range(FINE_COL // fit):
            value = None
            for part in range(fit):
                shift = (part - run) % fit * chunk
                plane = planes[half * fit + part]
                plane = pltpu.roll(plane, shift, 1) if shift else plane
                value = plane if part == 0 else jnp.where(lane >= part * chunk, plane, value)
            halves.append(value)
        mixed.append(jnp.concatenate(halves, axis=1))
    mixed = jnp.concatenate(mixed, axis=0)
    high = mixed.astype(BF16).astype(F32)
    mixed = jnp.concatenate([high, mixed - high], axis=0).astype(BF16)
    ordered = jnp.dot(mixed, perm_ref[...], preferred_element_type=F32)
    tile_tall = tile_rows + ROW_PAD
    runs = cols // span
    ordered = ordered[: runs * tile_tall] + ordered[runs * tile_tall :]
    natural = jnp.concatenate(
        [ordered[run * tile_tall : (run + 1) * tile_tall] for run in range(runs)], axis=1
    )
    tile_ref[:, :cols] = natural
    tile_ref[:, cols:] = beyond
    top = iota((ROW_PAD, cols + COL_PAD), 0) == 0
    pack_ref[...] = jnp.where(
        top, tile_ref[tile_rows:], tile_ref[tile_rows - ROW_PAD : tile_rows]
    )
    sides = jnp.where(lane < COL_PAD // 2, natural[:, :COL_PAD], natural[:, cols - COL_PAD :])
    sides = jnp.where(lane == COL_PAD - 8, pltpu.roll(beyond, COL_PAD - 8, 1), sides)
    sides = jnp.concatenate([sides, jnp.zeros((COL_PAD - tile_tall, COL_PAD), F32)], axis=0)
    strip_ref[...] = sides.T

    split = rows - ROW_PAD
    mine = pl.multiple_of(core * split, 8)
    theirs = pl.multiple_of((1 - core) * split, 8)
    north = lat > 0
    south = lat < n_lat - 1
    from_west = strip_ref.at[pl.ds(0, 8)]
    from_east = strip_ref.at[pl.ds(COL_PAD - 8, 8)]

    def swap_copy(out, into, source, target, device):
        return pltpu.make_async_remote_copy(
            src_ref=source,
            dst_ref=target,
            send_sem=swap_send.at[out],
            recv_sem=swap_recv.at[into],
            device_id=device,
            device_id_type=MESH,
        )

    up_lat, down_lat = jnp.maximum(lat - 1, 0), jnp.minimum(lat + 1, n_lat - 1)

    def northern():
        return [
            swap_copy(1, 1 + core, tile_ref.at[pl.ds(0, 8)], edge_ref.at[core], (up_lat, lon, 1)),
            swap_copy(2, 3 + core, from_west, side_ref.at[2 + core], (up_lat, west, 1)),
            swap_copy(3, 5 + core, from_east, side_ref.at[6 + core], (up_lat, east, 1)),
        ]

    def southern():
        return [
            swap_copy(4, 1 + core, pack_ref, edge_ref.at[core], (down_lat, lon, 0)),
            swap_copy(5, 3 + core, from_west, side_ref.at[2 + core], (down_lat, west, 0)),
            swap_copy(6, 5 + core, from_east, side_ref.at[6 + core], (down_lat, east, 0)),
        ]

    level = [
        swap_copy(7 + peer, 7 + core, from_west, side_ref.at[core], (lat, west, peer))
        for peer in range(2)
    ] + [
        swap_copy(9 + peer, 9 + core, from_east, side_ref.at[4 + core], (lat, east, peer))
        for peer in range(2)
    ]
    swap = swap_copy(0, 0, tile_ref.at[pl.ds(theirs, tall)], pair_ref, (lat, lon, 1 - core))

    @pl.when(north)
    def _():
        for item in northern():
            item.start()

    @pl.when(south)
    def _():
        for item in southern():
            item.start()

    for item in level:
        item.start()
    swap.start()

    mid_ref[:, inside] = ground_ref[...]

    @pl.when(line > 0)
    def _():
        for item in halo_below():
            item.wait_recv()

    @pl.when(line < last_line)
    def _():
        for item in halo_above():
            item.wait_recv()

    @pl.when(line == 0)
    def _():
        for ref in (mid_ref, cwest_ref, ceast_ref):
            ref[:, row_before] = jnp.zeros_like(ref[:, row_before])

    @pl.when(line == last_line)
    def _():
        for ref in (mid_ref, cwest_ref, ceast_ref):
            ref[:, row_after] = jnp.zeros_like(ref[:, row_after])

    for item in level_halo:
        item.wait_recv()
    near = iota((tall, COL_PAD), 1) < COL_PAD // 2

    def widened(index):
        pad = jnp.where(near, ceast_ref[index], cwest_ref[index])
        return jnp.concatenate([mid_ref[index], pad], axis=1)

    conduct = widened(0)
    cn = jnp.sqrt(conduct * moved(conduct, 0, False))
    cs = moved(cn, 0, True)
    cw = jnp.sqrt(conduct * moved(conduct, 1, False))
    ce = moved(cw, 1, True)
    cn_ref[...] = cn
    cs_ref[...] = cs
    cw_ref[...] = cw
    ce_ref[...] = ce
    ocean_ref[...] = jnp.where(conduct > 0.0, 1.0, 0.0)
    diag_ref[...] = widened(1) + cn + cs + cw + ce

    ocean_count, diag_sum, diag_square, face_square = take_sum(0, 4)
    ocean_count = jnp.maximum(ocean_count, 1.0)
    mean = diag_sum / ocean_count
    spread_out = jnp.maximum((diag_square + face_square) / ocean_count - mean * mean, 0.0)
    mean = 1.2 * mean

    def across(value, size):
        return jnp.concatenate([value] * (size // COL_PAD), axis=1)

    diag_ref[...] = diag_ref[...] - across(mean, cols + COL_PAD)

    def finish(k, carry):
        block_copy(k).wait_send()
        return carry

    lax.fori_loop(1, tiles, finish, 0)
    for item in level_halo:
        item.wait_send()

    @pl.when(line > 0)
    def _():
        for item in halo_above():
            item.wait_send()

    @pl.when(line < last_line)
    def _():
        for item in halo_below():
            item.wait_send()

    linked = jnp.where(core == 0, lat, n_lat - 1 - lat) > 0

    def arrived(number, target):
        return swap_copy(0, number, target, target, (lat, lon, 1 - core))

    @pl.when(linked)
    def _():
        for sender in range(2):
            arrived(1 + sender, edge_ref.at[sender]).wait_recv()
            arrived(3 + sender, side_ref.at[2 + sender]).wait_recv()
            arrived(5 + sender, side_ref.at[6 + sender]).wait_recv()

    @pl.when(jnp.logical_not(linked))
    def _():
        edge_ref[...] = jnp.zeros_like(edge_ref)
        side_ref[2:4] = jnp.zeros((2, 8, COL_PAD), F32)
        side_ref[6:8] = jnp.zeros((2, 8, COL_PAD), F32)

    for sender in range(2):
        arrived(7 + sender, side_ref.at[sender]).wait_recv()
        arrived(9 + sender, side_ref.at[4 + sender]).wait_recv()

    def aligned(straight, corner):
        first = core == 0
        straight = jnp.where(
            first, pltpu.roll(straight, ROW_PAD, 1), pltpu.roll(straight, COL_PAD - split, 1)
        )
        corner = jnp.where(
            first,
            pltpu.roll(corner, COL_PAD - (tile_rows - ROW_PAD), 1),
            pltpu.roll(corner, keep, 1),
        )
        return straight + corner

    right_side = aligned(side_ref[0] + side_ref[1], side_ref[2] + side_ref[3])
    left_side = aligned(side_ref[4] + side_ref[5], side_ref[6] + side_ref[7])
    hole = jnp.zeros((COL_PAD - 16, COL_PAD), F32)
    beside = jnp.concatenate([right_side, hole, left_side], axis=0).T[:tall]
    entering = jnp.where(iota(beside.shape, 1) == 0, pltpu.roll(beside, 8, 1), 0.0)
    edge = edge_ref[0] + edge_ref[1]
    swap.wait_recv()

    @pl.when(core == 0)
    def _():
        q_ref[0, :ROW_PAD] = jnp.where(top, 0.0, edge)
        q_ref[0, ROW_PAD : 2 * ROW_PAD] = (
            tile_ref[:ROW_PAD] + pair_ref[:ROW_PAD] + jnp.where(top, edge, 0.0)
        )
        q_ref[0, 2 * ROW_PAD :] = tile_ref[ROW_PAD:keep] + pair_ref[ROW_PAD:keep]

    @pl.when(core == 1)
    def _():
        q_ref[0, :keep] = tile_ref[pl.ds(split, keep)] + pair_ref[:keep]
        q_ref[0, keep:] = tile_ref[pl.ds(split + keep, ROW_PAD)] + pair_ref[keep:] + edge

    q_ref[0, :, :COL_PAD] = q_ref[0, :, :COL_PAD] + entering
    q_ref[0, :, cols:] = q_ref[0, :, cols:] + beside
    q_ref[0] = q_ref[0] * ocean_ref[...]

    spread_wide = across(spread_out, cols + COL_PAD)
    for k in range(ITERS):
        field = q_ref[k]
        value = (
            diag_ref[...] * field
            - cn_ref[...] * moved(field, 0, False)
            - cs_ref[...] * moved(field, 0, True)
            - cw_ref[...] * moved(field, 1, False)
            - ce_ref[...] * moved(field, 1, True)
        )
        if k:
            value = value - spread_wide * q_ref[k - 1]
        if k < ITERS - 1:
            q_ref[k + 1] = value
        else:
            q_ref[k + 1, ROW_PAD:keep, :cols] = value[ROW_PAD:keep, :cols]

    fields = [q_ref[k, ROW_PAD:keep, :cols] for k in range(ITERS + 1)]
    pairs = [(k, k + d) for k in range(ITERS) for d in range(2)]
    post_sum(1, [fold(fields[i] * fields[j]) for i, j in pairs])
    swap.wait_send()
    for item in level:
        item.wait_send()

    @pl.when(north)
    def _():
        for item in northern():
            item.wait_send()

    @pl.when(south)
    def _():
        for item in southern():
            item.wait_send()

    sums = take_sum(1, len(pairs))
    gram = {}
    for (i, j), value in zip(pairs, sums):
        gram[i, j] = gram[j, i] = value
    for gap in range(1, ITERS):
        for i in range(ITERS - gap):
            j = i + gap
            value = gram[i + 1, j]
            if i:
                value = value + spread_out * (gram[i - 1, j] - gram[i, j - 1])
            else:
                value = value - spread_out * gram[i, j - 1]
            gram[i, j + 1] = gram[j + 1, i] = value

    def plus(one, two):
        if one is None or two is None:
            return two if one is None else one
        return one + two

    def times(weight, part):
        return None if part is None else weight * part

    def quad(first, second):
        out = None
        for i, one in enumerate(first):
            line = None
            for j, two in enumerate(second):
                if one is not None and two is not None:
                    line = plus(line, two * gram[i, j])
            out = plus(out, times(one, line) if one is not None else None)
        return out

    def apply(weights):
        out = [None] * (ITERS + 1)
        for k, weight in enumerate(weights[:ITERS]):
            if weight is not None:
                out[k + 1] = plus(out[k + 1], weight)
                out[k] = plus(out[k], mean * weight)
                if k:
                    out[k - 1] = plus(out[k - 1], spread_out * weight)
        return out

    unit = jnp.ones((1, COL_PAD), F32)
    direct = [unit] + [None] * ITERS
    resid = [unit] + [None] * ITERS
    gained = [None] * (ITERS + 1)
    norm = gram[0, 0]
    for done in range(1, ITERS + 1):
        applied = apply(direct)
        step_size = norm / quad(direct, applied)
        gained = [plus(one, times(step_size, two)) for one, two in zip(gained, direct)]
        resid = [plus(one, times(-step_size, two)) for one, two in zip(resid, applied)]
        if done < ITERS:
            norm_next = quad(resid, resid)
            ratio = norm_next / norm
            direct = [plus(one, times(ratio, two)) for one, two in zip(resid, direct)]
            norm = norm_next

    def mix(weights):
        out = None
        for k, weight in enumerate(weights):
            if weight is not None:
                out = plus(out, across(weight, cols) * q_ref[k, ROW_PAD:keep, :cols])
        return out

    x_ref[...] = mix(gained)
    r_ref[...] = mix(resid)


def write(x_ref, r_ref, x_hbm, r_hbm, sem):
    copies = [
        pltpu.make_async_copy(x_ref, x_hbm, sem.at[0]),
        pltpu.make_async_copy(r_ref, r_hbm, sem.at[1]),
    ]
    for copy in copies:
        copy.start()
    for copy in copies:
        copy.wait()


def body(
    innovation, obs_error, obs_offset, obs_cell, obs_owner, block_count,
    land_mask, inertia, sea_depth,
):
    block_total = obs_owner.shape[1]
    width = innovation.shape[1]
    n_lat, n_lon, n_obs = (lax.axis_size(name) for name in AXES)
    tiles = n_lat * n_lon
    capacity = max(3, 2 * ((block_total + tiles - 1) // tiles))
    cap_pad = -(-capacity // 8) * 8
    rows, cols = land_mask.shape
    total = tiles * n_obs
    coarse = (rows * n_obs // FINE_ROW) * (cols // FINE_COL)
    tall, broad = rows + 2 * ROW_PAD, cols + COL_PAD
    tile_tall = rows * n_obs + ROW_PAD
    vmem = lambda *shape: pltpu.VMEM(shape, F32)
    whole = pl.BlockSpec(memory_space=pltpu.VMEM)
    far = pl.BlockSpec(memory_space=pltpu.HBM)
    dma = pltpu.SemaphoreType.DMA
    fields = pl.pallas_call(
        functools.partial(kernel, capacity),
        out_shape=[pltpu.VMEM((rows, cols), F32)] * 2,
        in_specs=[far] * 9,
        out_specs=[whole] * 2,
        scratch_shapes=[
            vmem(*innovation.shape),
            vmem(*obs_error.shape),
            vmem(*obs_offset.shape),
            pltpu.VMEM(obs_cell.shape, jnp.int32),
            pltpu.VMEM(obs_owner.shape, jnp.int32),
            pltpu.SMEM(block_count.shape, jnp.int32),
            pltpu.VMEM((rows, cols), jnp.int32),
            vmem(rows, cols),
            vmem(2, rows, cols),
            vmem(tiles, cap_pad, 4 * width),
            vmem(tiles + 1, cap_pad, 4 * width),
            vmem(2 * fine_size(), coarse),
            pltpu.VMEM((2 * COL_PAD, 2 * COL_PAD), BF16),
            vmem(tile_tall, broad),
            vmem(ROW_PAD, broad),
            vmem(COL_PAD, COL_PAD),
            vmem(tall, broad),
            vmem(2, ROW_PAD, broad),
            vmem(8, 8, COL_PAD),
            vmem(2, tall, cols),
            vmem(2, tall, COL_PAD),
            vmem(2, tall, COL_PAD),
        ]
        + [vmem(tall, broad)] * 6
        + [
            vmem(ITERS + 1, tall, broad),
            vmem(2, 1, COL_PAD),
            vmem(2, total, 1, COL_PAD),
            vmem(COL_PAD, COL_PAD),
            dma((9,)),
            dma((tiles,)),
            dma((tiles + 1,)),
            dma((8,)),
            dma((8,)),
            dma((11,)),
            dma((11,)),
            dma((2,)),
            dma((2,)),
        ],
        compiler_params=pltpu.CompilerParams(collective_id=0, has_side_effects=True),
        name="adjoint",
    )(
        innovation, obs_error, obs_offset, obs_cell, obs_owner, block_count,
        land_mask, inertia, sea_depth,
    )
    return pl.pallas_call(
        write,
        out_shape=[jax.ShapeDtypeStruct((rows, cols), F32)] * 2,
        in_specs=[whole] * 2,
        out_specs=[far] * 2,
        scratch_shapes=[dma((2,))],
        name="write",
    )(*[pltpu.with_memory_space_constraint(field, pltpu.VMEM) for field in fields])


def solution(mesh):
    spread = P(AXES, None)
    grid = P(("lat", "obs"), "lon")
    in_specs = (spread, spread, P(None, AXES, None), spread, spread, P(AXES), grid, grid, grid)
    return jax.shard_map(
        body, mesh=mesh, in_specs=in_specs, out_specs=(grid, grid), check_vma=False
    )
```
